32 devices in a mesh: pipe: 2 (over core), seq: 8 (over z, x), tp: 2 (over y).
Axes of the slice: x: 2, y: 2, z: 4, core: 2. Of those that a mesh axis runs over, the one named last changes fastest.
Arguments:
- hidden_in: bfloat16 [1, 4096, 2560], P(None, ('seq', 'tp')), may hold values from -6 to 6
- doc_ids: int32 [1, 4096], P(None, 'seq'), may hold values from 0 to 1, never falling along the last dimension, each value on 1 to 3072 neighbouring positions
- norm_gain: float32 [2, 2560], P('pipe'), may hold values from 0.1 to 1.9
- in_zx: bfloat16 [2, 2560, 2, 5120], P('pipe', None, None, 'tp'), may hold values from -0.125 to 0.125
- in_bc: bfloat16 [2, 2560, 256], P('pipe'), may hold values from -0.125 to 0.125
- in_dt: bfloat16 [2, 2560, 80], P('pipe', None, 'tp'), may hold values from -0.125 to 0.125
- conv_x: float32 [2, 4, 5120], P('pipe', None, 'tp'), may hold values from -3 to 3
- conv_bc: float32 [2, 4, 256], P('pipe'), may hold values from -3 to 3
- bias_x: float32 [2, 5120], P('pipe', 'tp'), may hold values from -3 to 3
- bias_bc: float32 [2, 256], P('pipe'), may hold values from -3 to 3
- dt_bias: float32 [2, 80], P('pipe', 'tp'), may hold values from -2 to 1
- a_log: float32 [2, 80], P('pipe', 'tp'), may hold values from -12 to 0, as said below
- d_skip: float32 [2, 80], P('pipe', 'tp'), may hold values from 0.5 to 1.5
- gated_gain: float32 [2, 5120], P('pipe', 'tp'), may hold values from 0.1 to 1.9
- out_w: bfloat16 [2, 5120, 2560], P('pipe', 'tp'), may hold values from -0.078125 to 0.078125
Outputs:
- section_out: bfloat16 [2, 1, 4096, 2560], P('pipe', None, ('seq', 'tp'))
The draws below stay inside these ranges and needn't reach their ends.
Inputs may be any that keep to these rules, and one draw needn't show every extreme that they name: `doc_ids`: in each row the document numbers start at 0, never fall, and rise by one where a new document begins; every document spans 1 to 3072 positions. `a_log`: logarithms of rates between 0.5 / 4096 and 1.
All inputs are finite; a program needn't handle non-finite values.
Results may differ from the reference program's by a relative error of at most 0.02.
Values may be sent and summed in bfloat16 or wider, within the bound.
No kernel may reach another device: no remote copies, remote signals or barrier semaphores. Data moves between devices by JAX's collectives and lax.ppermute only.
A program may use at most 192 MiB of HBM per device.

```python
import math
import jax
import jax.numpy as jnp
import numpy as np
from jax import lax

D = 2560
E = 5120
H = 80
HEADDIM = 64
NS = 128
KW = 4
BLOCK = 256
MB = 1
SEQLEN = 4096
LAYERS = 2


def draw_a_log(key, part):
    uniform_draw = jax.random.uniform(key, (LAYERS, H), jnp.float32)
    lowest = math.log(0.5 / SEQLEN)
    return (lowest * (1.0 - uniform_draw)).astype(jnp.float32)


def block_scale(stream_key, extent, pieces, least, high):
    def one(axis_at, blocks):
        steps = jax.random.uniform(jax.random.fold_in(jax.random.fold_in(stream_key, 6), axis_at), (blocks,), jnp.float32, least / len(pieces), high / len(pieces))
        return jnp.repeat(jnp.exp(steps), extent[axis_at] // blocks).reshape((-1,) + (1,) * (len(extent) - axis_at - 1))

    loudness = one(*pieces[0])
    for cut in pieces[1:]:
        loudness = loudness * one(*cut)
    return loudness


def profile(count, total, bound, slope):
    portions = [(1 << 20) // math.isqrt(standing ** slope) + 1 for standing in range(2, count + 1)]
    spare, given = total - bound - (count - 1), [1] * (count - 1)
    while spare > 0:
        movable = [i for i in range(count - 1) if given[i] < bound]
        whole, remaining = sum([portions[i] for i in movable]), spare
        for i in movable:
            addition = min(bound - given[i], max(1, remaining * portions[i] // whole), spare)
            given[i] = given[i] + addition
            spare = spare - addition
    return np.array([bound] + given)


def uneven(own_key, number_of, total, limit, lean):
    if number_of == 2:
        one = jax.random.randint(own_key, (), max(1, total - limit), min(limit, total - 1) + 1)
        return jnp.stack([one, total - one])
    tallies = jnp.asarray(profile(number_of, total, limit, lean), jnp.int32)
    couples = (number_of - 1) // 2
    source_of, taker = tallies[1:1 + 2 * couples:2], tallies[2:2 + 2 * couples:2]
    slack = jnp.minimum(source_of - 1, limit - taker)
    passed = jax.random.randint(jax.random.fold_in(own_key, 1), (couples,), 0, 1 << 20) % (slack + 1)
    tallies = tallies.at[1:1 + 2 * couples:2].set(source_of - passed).at[2:2 + 2 * couples:2].set(taker + passed)
    return tallies[jax.random.permutation(jax.random.fold_in(own_key, 2), number_of)]


def gaussian(key, extent, scale, bound, shards=(), dtype=jnp.bfloat16):
    entries = scale * jax.random.normal(key, extent, jnp.float32)
    if shards:
        entries = entries * block_scale(key, extent, shards, -0.22, 0.18)
    return jnp.clip(entries, -bound, bound).astype(dtype)


def setup_inputs(seed: int = 0) -> dict:
    arg_keys = jax.random.split(jax.random.key(seed), 16)
    hidden_in = gaussian(arg_keys[0], (MB, SEQLEN, D), 1.0, 6.0, ((1, 16),))
    doc_ids = jax.vmap(lambda own: jnp.searchsorted(jnp.cumsum(uneven(own, 2, SEQLEN, 3 * SEQLEN // 4, 0)), jnp.arange(SEQLEN), side="right"))(jax.random.split(arg_keys[1], MB)).reshape((MB, SEQLEN)).astype(jnp.int32)
    norm_gain = jnp.clip(1.0 + 0.18 * jax.random.normal(arg_keys[2], (LAYERS, D), jnp.float32), 0.1, 1.9)
    in_zx = gaussian(arg_keys[3], (LAYERS, D, 2, E), D ** -0.5, 0.125, ((0, 2), (3, 2)))
    in_bc = gaussian(arg_keys[4], (LAYERS, D, 2 * NS), D ** -0.5, 0.125, ((0, 2),))
    in_dt = gaussian(arg_keys[5], (LAYERS, D, H), D ** -0.5, 0.125, ((0, 2), (2, 2)))
    conv_x = gaussian(arg_keys[6], (LAYERS, KW, E), KW ** -0.5, 3.0, ((0, 2), (2, 2)), jnp.float32)
    conv_bc = gaussian(arg_keys[7], (LAYERS, KW, 2 * NS), KW ** -0.5, 3.0, ((0, 2),), jnp.float32)
    bias_x = gaussian(arg_keys[8], (LAYERS, E), 0.5, 3.0, ((0, 2), (1, 2)), jnp.float32)
    bias_bc = gaussian(arg_keys[9], (LAYERS, 2 * NS), 0.5, 3.0, ((0, 2),), jnp.float32)
    dt_bias = jnp.clip(-2.0 + 3.0 * jax.random.uniform(arg_keys[10], (LAYERS, H), jnp.float32) ** block_scale(arg_keys[10], (LAYERS, H), ((0, 2), (1, 2)), -0.2, 0.2), -2.0, 1.0)
    a_log = draw_a_log(jax.random.fold_in(arg_keys[15], 71), 0)
    d_skip = jnp.clip(0.5 + 1.0 * jax.random.uniform(arg_keys[12], (LAYERS, H), jnp.float32) ** block_scale(arg_keys[12], (LAYERS, H), ((0, 2), (1, 2)), -0.2, 0.2), 0.5, 1.5)
    gated_gain = jnp.clip(1.0 + 0.18 * jax.random.normal(arg_keys[13], (LAYERS, E), jnp.float32), 0.1, 1.9)
    out_w = gaussian(arg_keys[14], (LAYERS, E, D), E ** -0.5, 0.078125, ((0, 2), (1, 2)))
    return dict(hidden_in=hidden_in, doc_ids=doc_ids, norm_gain=norm_gain, in_zx=in_zx, in_bc=in_bc, in_dt=in_dt, conv_x=conv_x, conv_bc=conv_bc, bias_x=bias_x, bias_bc=bias_bc, dt_bias=dt_bias, a_log=a_log, d_skip=d_skip, gated_gain=gated_gain, out_w=out_w)


epsilon = 1e-05
highest = lax.Precision.HIGHEST

def conv_mix(row_block, edge_rows, row_ids, edge_ids, weight, shift_bias):
    padded = jnp.concatenate([edge_rows, row_block], 0)
    padded_ids = jnp.concatenate([edge_ids, row_ids], 0)
    row_count = row_block.shape[0]
    running = jnp.zeros_like(row_block) + shift_bias[None, :]
    for offset in range(weight.shape[0]):
        keep_mask = (padded_ids[offset:offset + row_count] == row_ids).astype(jnp.float32)
        running = running + keep_mask[:, None] * weight[offset][None, :] * padded[offset:offset + row_count]
    return jax.nn.silu(running)

def block_step(state_in, inputs, decay_rates):
    x_block, step_sizes, b_block, c_block, seg_block, prev_id = inputs
    log_decay = jnp.cumsum(step_sizes * decay_rates[:, None], axis=1)
    block_length = seg_block.shape[0]
    causal_mask = jnp.arange(block_length)[:, None] >= jnp.arange(block_length)[None, :]
    same_doc = causal_mask & (seg_block[:, None] == seg_block[None, :])
    spread = log_decay[:, :, None] - log_decay[:, None, :]
    mixing = jnp.where(same_doc[None], jnp.exp(jnp.where(same_doc[None], spread, 0.0)), 0.0)
    gram_matrix = jnp.dot(c_block, b_block.T, precision=highest)
    weights = mixing * gram_matrix[None] * step_sizes[:, None, :]
    outputs = jnp.einsum('hps,hts->hpt', x_block, weights, precision=highest)
    carried = (seg_block == prev_id).astype(jnp.float32)
    outputs = outputs + jnp.exp(log_decay)[:, None, :] * carried[None, None, :] * jnp.einsum('hpn,tn->hpt', state_in, c_block, precision=highest)
    end_weight = jnp.exp(log_decay[:, -1:] - log_decay) * (seg_block == seg_block[-1]).astype(jnp.float32)[None, :] * step_sizes
    fresh_state = jnp.einsum('hps,sn->hpn', x_block * end_weight[:, None, :], b_block, precision=highest)
    keep_all = jnp.exp(log_decay[:, -1]) * (seg_block[-1] == prev_id).astype(jnp.float32)
    return (keep_all[:, None, None] * state_in + fresh_state, outputs)

def mamba_layer(hidden, row_ids, norm_scale, weight_zx, weight_bc, weight_dt, kernel_x, kernel_bc, offset_x, offset_bc, dt_shift, log_rate, skip_scale, gate_scale, weight_out):
    hidden_f = hidden.astype(jnp.float32)
    normed = (hidden_f * lax.rsqrt(lax.optimization_barrier(jnp.mean(hidden_f * hidden_f, axis=1, keepdims=True)) + epsilon) * norm_scale[None, :]).astype(jnp.bfloat16)
    gate_in = jnp.dot(normed, weight_zx[:, 0, :], preferred_element_type=jnp.float32)
    x_raw = jnp.dot(normed, weight_zx[:, 1, :], preferred_element_type=jnp.float32)
    bc_raw = jnp.dot(normed, weight_bc, preferred_element_type=jnp.float32)
    dt_raw = jnp.dot(normed, weight_dt, preferred_element_type=jnp.float32)
    pre_conv = jnp.concatenate([x_raw, bc_raw], 1)
    kernel = jnp.concatenate([kernel_x, kernel_bc], 1)
    kernel_bias = jnp.concatenate([offset_x, offset_bc], 0)
    edge_rows = jnp.zeros((KW - 1, E + 2 * NS), jnp.float32)
    edge_ids = jnp.full((KW - 1,), -1, jnp.int32)
    conv_out = conv_mix(pre_conv, edge_rows, row_ids, edge_ids, kernel, kernel_bias)
    x_heads = conv_out[:, :E].T.reshape(H, HEADDIM, SEQLEN)
    b_conv = conv_out[:, E:E + NS]
    c_conv = conv_out[:, E + NS:]
    step_sizes = jax.nn.softplus(dt_raw + dt_shift[None, :]).T
    decay_rates = -jnp.exp(log_rate)
    blocks = SEQLEN // BLOCK
    prev_ids = jnp.concatenate([row_ids[:1], row_ids[BLOCK - 1:SEQLEN - 1:BLOCK]], 0)
    stacked = (x_heads.reshape(H, HEADDIM, blocks, BLOCK).transpose(2, 0, 1, 3), step_sizes.reshape(H, blocks, BLOCK).transpose(1, 0, 2), b_conv.reshape(blocks, BLOCK, NS), c_conv.reshape(blocks, BLOCK, NS), row_ids.reshape(blocks, BLOCK), prev_ids)

    def scan_body(state_in, inputs):
        return block_step(state_in, inputs, decay_rates)
    final_state, outputs = lax.scan(scan_body, jnp.zeros((H, HEADDIM, NS), jnp.float32), stacked)
    outputs = outputs.transpose(1, 2, 0, 3).reshape(H, HEADDIM, SEQLEN)
    outputs = outputs + skip_scale[:, None, None] * x_heads
    gated_rows = outputs.reshape(E, SEQLEN).T * jax.nn.silu(gate_in)
    branch_in = (gated_rows * lax.rsqrt(lax.optimization_barrier(jnp.mean(gated_rows * gated_rows, axis=1, keepdims=True)) + epsilon) * gate_scale[None, :]).astype(jnp.bfloat16)
    return (hidden_f + jnp.dot(branch_in, weight_out, preferred_element_type=jnp.float32)).astype(jnp.bfloat16)

def reference(hidden_in, doc_ids, norm_gain, in_zx, in_bc, in_dt, conv_x, conv_bc, bias_x, bias_bc, dt_bias, a_log, d_skip, gated_gain, out_w):
    per_layer = [[None] * MB for layer_index in range(LAYERS)]
    for micro_index in range(MB):
        hidden = hidden_in[micro_index]
        row_ids = doc_ids[micro_index]
        for layer_index in range(LAYERS):
            hidden = mamba_layer(hidden, row_ids, norm_gain[layer_index], in_zx[layer_index], in_bc[layer_index], in_dt[layer_index], conv_x[layer_index], conv_bc[layer_index], bias_x[layer_index], bias_bc[layer_index], dt_bias[layer_index], a_log[layer_index], d_skip[layer_index], gated_gain[layer_index], out_w[layer_index])
            per_layer[layer_index][micro_index] = hidden
    return jnp.stack([jnp.stack(micro_list) for micro_list in per_layer])
```

```python
import functools

import jax
import jax.numpy as jnp
from jax import lax
from jax.experimental import pallas as pl
from jax.experimental.pallas import tpu as pltpu
from jax.sharding import PartitionSpec as P

AXES = ("pipe", "seq", "tp")
BLOCK = 256
HALO = 16
KEEP_ROWS = 16
LANES = 128
epsilon = 1e-05
highest = lax.Precision.HIGHEST
f32 = jnp.float32
bf16 = jnp.bfloat16


def dot(a, b):
    return jnp.dot(a, b, preferred_element_type=f32)


def cost(micros):
    return pl.CostEstimate(flops=int(micros * 2.5e8), bytes_accessed=0, transcendentals=0)


def silu(v):
    half = 0.5 * v
    return half + half * jnp.tanh(half)


def softplus(v):
    return jnp.maximum(v, 0.0) + jnp.log1p(jnp.exp(-jnp.abs(v)))


def spread_matrix(heads, width, tile):
    rows = lax.broadcasted_iota(jnp.int32, (LANES, heads * width), 0) - tile * heads
    cols = lax.broadcasted_iota(jnp.int32, (LANES, heads * width), 1)
    inside = (cols >= rows * width) & (cols < (rows + 1) * width)
    return jnp.where(inside, 1.0, 0.0).astype(bf16)


def conv_rows(raw_ref, keep_ref, taps, bias, start, stop, col):
    width = LANES
    out = bias + taps[3:4] * raw_ref[start + 8 : stop + 8, col : col + width]
    for tap in range(3):
        shifted_rows = raw_ref[start + 5 + tap : stop + 5 + tap, col : col + width]
        out = out + keep_ref[tap, start:stop] * (taps[tap : tap + 1] * shifted_rows)
    return silu(out)


def scan_kernel(rows, heads, width, shares, at_ref, *refs):
    part_refs, halo_refs = refs[:shares], refs[shares : 2 * shares]
    (
        gain_ref,
        small_ref,
        wx_ref,
        tapx_ref,
        tapbc_ref,
        biasx_ref,
        biasbc_ref,
        dtb_ref,
        rate_ref,
        idc_ref,
        lhs,
        x_ref,
        xs_ref,
        bc_ref,
        acol_ref,
        arow_ref,
        ein_ref,
        eall_ref,
        state_ref,
        sent_ref,
        raw,
        keep,
        stepc,
        wend,
        kept,
    ) = refs[2 * shares :]
    step_at = pl.program_id(0)
    blocks = rows // BLOCK
    state_width = bc_ref.shape[1] // 2
    tile_lanes = heads * width
    unit = 256 if tile_lanes % 256 == 0 else LANES
    units = tile_lanes // unit

    @pl.when(step_at == 0)
    def _():
        gain = gain_ref[...]

        def normalize(part):
            scale = lax.rsqrt(jnp.mean(part * part, axis=1, keepdims=True) + epsilon)
            return (part * scale * gain).astype(bf16)

        for share in range(shares):
            for begin in range(0, rows // shares, HALO):
                place = pl.multiple_of(at_ref[share] + begin, HALO)
                part = part_refs[share][begin : begin + HALO].astype(f32)
                lhs[pl.ds(place, HALO)] = normalize(part)
        halo = halo_refs[0][...].astype(f32)
        for other in halo_refs[1:]:
            halo = halo + other[...].astype(f32)
        lhs[rows:] = normalize(halo)
        small = dot(lhs[...], small_ref[...])
        for tap in range(3):
            keep[tap] = (idc_ref[5 + tap : 5 + tap + rows] == idc_ref[8 : 8 + rows]).astype(f32)
        raw[0:8, 0 : 2 * state_width] = small[rows + HALO - 8 :, : 2 * state_width]
        raw[8 : 8 + rows, 0 : 2 * state_width] = small[:rows, : 2 * state_width]
        for col in range(0, 2 * state_width, LANES):
            bc_ref[:, col : col + LANES] = conv_rows(
                raw,
                keep,
                tapbc_ref[:, col : col + LANES],
                biasbc_ref[:, col : col + LANES],
                0,
                rows,
                col,
            ).astype(bf16)
        step = softplus(small[:rows, 2 * state_width :] + dtb_ref[...])
        log_step = step * rate_ref[...]
        at = lax.broadcasted_iota(jnp.int32, (BLOCK, BLOCK), 0)
        to = lax.broadcasted_iota(jnp.int32, (BLOCK, BLOCK), 1)
        lower = (at >= to).astype(f32)
        first_prev = idc_ref[7:8]
        before = jnp.zeros((1, LANES), f32)
        kept[...] = jnp.zeros_like(kept)
        for block in range(blocks):
            r0, r1 = block * BLOCK, (block + 1) * BLOCK
            ids = idc_ref[8 + r0 : 8 + r1]
            prev = idc_ref[7 + r0 : 8 + r0]
            last = idc_ref[7 + r1 : 8 + r1]
            part_step = step[r0:r1]
            total = jnp.dot(lower, log_step[r0:r1], precision=highest, preferred_element_type=f32)
            end = total[BLOCK - 1 : BLOCK]
            acol_ref[r0:r1] = total
            arow_ref[:, r0:r1] = total.T
            ein_ref[r0:r1] = (jnp.exp(total) * (ids == prev).astype(f32)).astype(bf16)
            eall_ref[r0:r1] = (jnp.exp(total + before) * (ids == first_prev).astype(f32)).astype(
                bf16
            )
            stepc[r0:r1] = part_step.astype(bf16)
            wend[r0:r1] = (jnp.exp(end - total) * (ids == last).astype(f32) * part_step).astype(
                bf16
            )
            kept[block : block + 1] = jnp.exp(end) * (last == prev).astype(f32)
            before = before + end
        kept[blocks : blocks + 1] = jnp.exp(before) * (
            idc_ref[7 + rows : 8 + rows] == first_prev
        ).astype(f32)

    spread = spread_matrix(heads, width, step_at)
    kept_now = kept[...]
    high = kept_now.astype(bf16)
    low = (kept_now - high.astype(f32)).astype(bf16)
    keep_lanes = dot(high, spread) + dot(low, spread)
    step_lanes = dot(stepc[...], spread)
    wend_lanes = dot(wend[...], spread)
    for u in range(units):
        cols = slice(u * unit, (u + 1) * unit)
        fresh = dot(lhs[...], wx_ref[:, cols])
        raw[0:8, cols] = fresh[rows + HALO - 8 :]
        raw[8 : 8 + rows, cols] = fresh[:rows]
    at = lax.broadcasted_iota(jnp.int32, (KEEP_ROWS, unit), 0)
    for u in range(units):
        cols = slice(u * unit, (u + 1) * unit)
        running = None
        for block in range(blocks):
            r0, r1 = block * BLOCK, (block + 1) * BLOCK
            pieces = []
            for col in range(u * unit, (u + 1) * unit, LANES):
                x_now = conv_rows(
                    raw,
                    keep,
                    tapx_ref[:, col : col + LANES],
                    biasx_ref[:, col : col + LANES],
                    r0,
                    r1,
                    col,
                )
                x_ref[r0:r1, col : col + LANES] = x_now.astype(bf16)
                xs_ref[r0:r1, col : col + LANES] = (
                    x_now * step_lanes[r0:r1, col : col + LANES]
                ).astype(bf16)
                pieces.append((x_now * wend_lanes[r0:r1, col : col + LANES]).astype(bf16))
            local = lax.dot_general(
                bc_ref[r0:r1, 0:state_width],
                jnp.concatenate(pieces, 1),
                (((0,), (0,)), ((), ())),
                preferred_element_type=f32,
            )
            if running is not None:
                local = local + keep_lanes[block : block + 1, cols] * running
            running = local
            if block < blocks - 1:
                state_ref[block, :, cols] = running.astype(bf16)
        sent_ref[0:state_width, cols] = running.astype(bf16)
        shard_row = keep_lanes[blocks : blocks + 1, cols]
        shard_high = shard_row.astype(bf16).astype(f32)
        both = jnp.where(
            at == 0, shard_high, jnp.where(at == 1, shard_row - shard_high, 0.0)
        )
        sent_ref[state_width:, cols] = both.astype(bf16)


def scan_call(at, parts, halos, gain, small, w_zx, tapx, tapbc, biasx, biasbc, dtb, rate, idc, sizes):
    rows, heads, width, tiles, state_width = sizes
    shares, depth = len(parts), w_zx.shape[0]
    tile_lanes = heads * width
    channels = tiles * tile_lanes
    blocks = rows // BLOCK

    def whole(*shape):
        return pl.BlockSpec(shape, lambda i, at: (0,) * len(shape))

    def column(lead):
        return pl.BlockSpec((lead, tile_lanes), lambda i, at: (0, i))

    return pl.pallas_call(
        functools.partial(scan_kernel, rows, heads, width, shares),
        grid_spec=pltpu.PrefetchScalarGridSpec(
            num_scalar_prefetch=1,
            grid=(tiles,),
            in_specs=[whole(rows // shares, depth)] * shares
            + [whole(HALO, depth)] * shares
            + [
                whole(1, depth),
                whole(depth, 2 * state_width + LANES),
                pl.BlockSpec((depth, tile_lanes), lambda i, at: (0, tiles + i)),
                column(4),
                whole(4, 2 * state_width),
                column(1),
                whole(1, 2 * state_width),
                whole(1, LANES),
                whole(1, LANES),
                whole(rows + 8, LANES),
            ],
            out_specs=[
                whole(rows + HALO, depth),
                column(rows),
                column(rows),
                whole(rows, 2 * state_width),
                whole(rows, LANES),
                whole(LANES, rows),
                whole(rows, LANES),
                whole(rows, LANES),
                pl.BlockSpec(
                    (max(blocks - 1, 1), state_width, tile_lanes), lambda i, at: (0, 0, i)
                ),
                column(state_width + KEEP_ROWS),
            ],
            scratch_shapes=[
                pltpu.VMEM((rows + 8, max(tile_lanes, 2 * state_width)), f32),
                pltpu.VMEM((3, rows, LANES), f32),
                pltpu.VMEM((rows, LANES), bf16),
                pltpu.VMEM((rows, LANES), bf16),
                pltpu.VMEM((max(8, blocks + 1), LANES), f32),
            ],
        ),
        out_shape=[
            jax.ShapeDtypeStruct((rows + HALO, depth), bf16),
            jax.ShapeDtypeStruct((rows, channels), bf16),
            jax.ShapeDtypeStruct((rows, channels), bf16),
            jax.ShapeDtypeStruct((rows, 2 * state_width), bf16),
            jax.ShapeDtypeStruct((rows, LANES), f32),
            jax.ShapeDtypeStruct((LANES, rows), f32),
            jax.ShapeDtypeStruct((rows, LANES), bf16),
            jax.ShapeDtypeStruct((rows, LANES), bf16),
            jax.ShapeDtypeStruct((max(blocks - 1, 1), state_width, channels), bf16),
            jax.ShapeDtypeStruct((state_width + KEEP_ROWS, channels), bf16),
        ],
        compiler_params=pltpu.CompilerParams(
            dimension_semantics=("arbitrary",), vmem_limit_bytes=60 * 2**20
        ),
        cost_estimate=cost(15),
        name="scan",
    )(at, *parts, *halos, gain, small, w_zx, tapx, tapbc, biasx, biasbc, dtb, rate, idc)


def inner_kernel(
    rows,
    heads,
    width,
    x_ref,
    xs_ref,
    bc_ref,
    acol_ref,
    arow_ref,
    ein_ref,
    state_ref,
    skip_ref,
    idc_ref,
    idr_ref,
    y_ref,
    gram,
):
    blocks = rows // BLOCK
    state_width = bc_ref.shape[1] // 2

    @pl.when(pl.program_id(0) == 0)
    def _():
        at = lax.broadcasted_iota(jnp.int32, (BLOCK, BLOCK), 0)
        to = lax.broadcasted_iota(jnp.int32, (BLOCK, BLOCK), 1)
        for block in range(blocks):
            r0, r1 = block * BLOCK, (block + 1) * BLOCK
            b_rows = bc_ref[r0:r1, 0:state_width]
            c_rows = bc_ref[r0:r1, state_width:]
            ids = jnp.concatenate([idc_ref[8 + r0 : 8 + r1]] * (BLOCK // LANES), 1)
            same = (at >= to) & (ids == idr_ref[0:1, r0:r1])
            product = lax.dot_general(
                c_rows, b_rows, (((1,), (1,)), ((), ())), preferred_element_type=f32
            )
            gram[block] = jnp.where(same, product, 0.0)

    tile = pl.program_id(0)
    spread = spread_matrix(heads, width, tile)
    acol = pltpu.roll(acol_ref[...], lax.rem(LANES - tile * heads, LANES), 1)
    lane = lax.broadcasted_iota(jnp.int32, (BLOCK, LANES), 1)
    pack = LANES // width
    for block in range(blocks):
        r0, r1 = block * BLOCK, (block + 1) * BLOCK
        if block > 0:
            carried = dot(bc_ref[r0:r1, state_width:], state_ref[block - 1])
            carried = carried * dot(ein_ref[r0:r1], spread)
        for first in range(0, heads, pack):
            cols = slice(first * width, (first + pack) * width)
            xs_now = xs_ref[r0:r1, cols]
            total = None
            for inner in range(pack):
                head = first + inner
                gap = acol[r0:r1, head : head + 1] - arow_ref[head : head + 1, r0:r1]
                mix = (jnp.exp(jnp.minimum(gap, 0.0)) * gram[block]).astype(bf16)
                part = dot(mix, xs_now)
                total = part if total is None else jnp.where(lane < inner * width, total, part)
            total = total + skip_ref[:, cols] * x_ref[r0:r1, cols].astype(f32)
            if block > 0:
                total = total + carried[:, cols]
            y_ref[r0:r1, cols] = total.astype(bf16)


def inner_call(x, xs, bc, acol, arow, ein, states, skip, idc, idr, sizes):
    rows, heads, width, tiles, state_width = sizes
    tile_lanes = heads * width
    channels = tiles * tile_lanes
    blocks = rows // BLOCK

    def whole(*shape):
        return pl.BlockSpec(shape, lambda i: (0,) * len(shape))

    def column(lead):
        return pl.BlockSpec((lead, tile_lanes), lambda i: (0, i))

    arow_rows = heads if heads % 8 == 0 else LANES

    return pl.pallas_call(
        functools.partial(inner_kernel, rows, heads, width),
        grid=(tiles,),
        in_specs=[
            column(rows),
            column(rows),
            whole(rows, 2 * state_width),
            whole(rows, LANES),
            pl.BlockSpec((arow_rows, rows), lambda i: (i, 0)),
            whole(rows, LANES),
            pl.BlockSpec((max(blocks - 1, 1), state_width, tile_lanes), lambda i: (0, 0, i)),
            column(1),
            whole(rows + 8, LANES),
            whole(8, rows),
        ],
        out_specs=column(rows),
        out_shape=jax.ShapeDtypeStruct((rows, channels), bf16),
        scratch_shapes=[pltpu.VMEM((blocks, BLOCK, BLOCK), f32)],
        compiler_params=pltpu.CompilerParams(
            dimension_semantics=("arbitrary",), vmem_limit_bytes=60 * 2**20
        ),
        cost_estimate=cost(11),
        name="inner",
    )(x, xs, bc, acol, arow, ein, states, skip, idc, idr)


def gate_kernel(normed_ref, wz_ref, gate_ref):
    gate_ref[...] = silu(dot(normed_ref[...], wz_ref[...])).astype(bf16)


def gate_call(normed, w_zx, sizes):
    rows, heads, width, tiles, _ = sizes
    depth = normed.shape[1]
    tile_lanes = heads * width
    return pl.pallas_call(
        gate_kernel,
        grid=(tiles,),
        in_specs=[
            pl.BlockSpec((rows, depth), lambda i: (0, 0)),
            pl.BlockSpec((depth, tile_lanes), lambda i: (0, i)),
        ],
        out_specs=pl.BlockSpec((rows, tile_lanes), lambda i: (0, i)),
        out_shape=jax.ShapeDtypeStruct((rows, tiles * tile_lanes), bf16),
        compiler_params=pltpu.CompilerParams(
            dimension_semantics=("arbitrary",), vmem_limit_bytes=60 * 2**20
        ),
        cost_estimate=cost(8),
        name="gate",
    )(normed, w_zx)


def out_kernel(
    heads,
    width,
    tiles,
    at_ref,
    y_ref,
    gate_ref,
    bc_ref,
    eall_ref,
    stay_ref,
    got_ref,
    gain_ref,
    w_ref,
    p_ref,
    sq_ref,
    lhs,
    coming,
):
    state_width = bc_ref.shape[1] // 2
    tile_lanes = heads * width
    half = stay_ref.shape[1]

    @pl.when(pl.program_id(0) == 0)
    def _():
        swapped = at_ref[1] != 0
        coming[:, :half] = jnp.where(swapped, got_ref[...], stay_ref[...])
        coming[:, half:] = jnp.where(swapped, stay_ref[...], got_ref[...])
        squares = None
        for tile in range(tiles):
            cols = slice(tile * tile_lanes, (tile + 1) * tile_lanes)
            carried = dot(bc_ref[:, state_width:], coming[:, cols])
            carried = carried * dot(eall_ref[...], spread_matrix(heads, width, tile))
            gated = (y_ref[:, cols].astype(f32) + carried) * gate_ref[:, cols].astype(f32)
            part = jnp.sum(gated * gated, axis=1, keepdims=True)
            squares = part if squares is None else squares + part
            lhs[:, cols] = (gated * gain_ref[:, cols]).astype(bf16)
        sq_ref[...] = jnp.broadcast_to(squares, sq_ref.shape)

    p_ref[...] = dot(lhs[...], w_ref[...]).astype(bf16)


def out_call(at, y, gate, bc, eall, stay, got, gain, w_out, count, sizes):
    rows, heads, width, tiles, state_width = sizes
    channels, depth = w_out.shape
    piece = 512 if depth % 512 == 0 else depth

    def taken(lanes):
        return pl.BlockSpec((count, lanes), lambda i, at: (at[0], 0))

    def whole(*shape):
        return pl.BlockSpec(shape, lambda i, at: (0,) * len(shape))

    return pl.pallas_call(
        functools.partial(out_kernel, heads, width, tiles),
        grid_spec=pltpu.PrefetchScalarGridSpec(
            num_scalar_prefetch=1,
            grid=(depth // piece,),
            in_specs=[
                taken(channels),
                taken(channels),
                taken(2 * state_width),
                taken(LANES),
                whole(state_width, channels // 2),
                whole(state_width, channels // 2),
                whole(1, channels),
                pl.BlockSpec((channels, piece), lambda i, at: (0, i)),
            ],
            out_specs=[
                pl.BlockSpec((count, piece), lambda i, at: (0, i)),
                whole(count, LANES),
            ],
            scratch_shapes=[
                pltpu.VMEM((count, channels), bf16),
                pltpu.VMEM((state_width, channels), bf16),
            ],
        ),
        out_shape=[
            jax.ShapeDtypeStruct((count, depth), bf16),
            jax.ShapeDtypeStruct((count, LANES), f32),
        ],
        compiler_params=pltpu.CompilerParams(
            dimension_semantics=("arbitrary",), vmem_limit_bytes=60 * 2**20
        ),
        cost_estimate=cost(6),
        name="outp",
    )(at, y, gate, bc, eall, stay, got, gain, w_out)


class Route:
    def __init__(self, sizes):
        self.pipes, self.seqs, self.tps = sizes

    def spot(self, pipe, seq, tp):
        return (pipe * self.seqs + seq) * self.tps + tp

    def move(self, block, pairs):
        return lax.ppermute(
            block, AXES, [(self.spot(*source), self.spot(*target)) for source, target in pairs]
        )

    def every(self):
        return [(s, t) for s in range(self.seqs) for t in range(self.tps)]


def gather_rows(route, own, source_pipe, pipe, tail_after=None, ids_row=None):
    tps, seqs = route.tps, route.seqs
    parts = [own]
    if source_pipe != pipe:
        parts = [route.move(own, [((source_pipe, s, t), (pipe, s, t)) for s, t in route.every()])]
    for distance in range(1, tps):
        parts.append(
            route.move(
                own,
                [
                    ((source_pipe, s, (t + distance) % tps), (pipe, s, t))
                    for s, t in route.every()
                ],
            )
        )
    tail = own[own.shape[0] - HALO :]
    if ids_row is not None:
        tail = jnp.concatenate([tail, ids_row], 0)
    pipes = [(source_pipe, pipe)] if ids_row is None else [(p, p) for p in range(route.pipes)]
    halos = [
        route.move(
            tail,
            [((a, s, tps - 1), (b, s + 1, t)) for a, b in pipes for s in range(seqs - 1)],
        )
        for t in range(tps)
    ]
    return parts, halos


def exchange_states(route, sent, state_width, pipe, under_swap, under_scan, scan_inputs):
    seqs = route.seqs
    outer, side = seqs // 2, lax.axis_index("seq") % 2
    half = sent.shape[1] // 2
    is_first = side == 0

    def swap(block):
        return route.move(
            block, [((pipe, s, t), (pipe, s + 1 - 2 * (s % 2), t)) for s, t in route.every()]
        )

    def parted(block):
        block = block.astype(f32)
        keep = block[state_width : state_width + 1] + block[state_width + 1 : state_width + 2]
        return block[:state_width], keep

    def joined(state, keep):
        high = keep.astype(bf16)
        low = (keep - high.astype(f32)).astype(bf16)
        rest = jnp.zeros((KEEP_ROWS - 2, half), bf16)
        return jnp.concatenate([state.astype(bf16), high, low, rest], 0)

    low, high = sent[:, :half], sent[:, half:]
    mine = jnp.where(is_first, low, high)
    theirs = swap(jnp.where(is_first, high, low))
    theirs, gate = lax.optimization_barrier((theirs, under_swap()))
    early, keep_early = parted(jnp.where(is_first, mine, theirs))
    late, keep_late = parted(jnp.where(is_first, theirs, mine))
    pair = joined(keep_late * early + late, keep_early * keep_late)
    pair, scan_inputs = lax.optimization_barrier((pair, scan_inputs))
    arrivals = []
    for distance in range(1, outer):
        pairs = [
            ((pipe, s - 2 * distance, t), (pipe, s, t))
            for s, t in route.every()
            if s - 2 * distance >= 0
        ]
        arrivals.append(route.move(pair, pairs))
    arrivals, mixed = lax.optimization_barrier((arrivals, under_scan(*scan_inputs)))
    total, weight = parted(arrivals[0])
    for came in arrivals[1:]:
        came, keep_came = parted(came)
        total = total + weight * came
        weight = weight * keep_came
    after_early = keep_early * total + early
    stay = jnp.where(is_first, total, after_early).astype(bf16)
    got = swap(jnp.where(is_first, after_early, total).astype(bf16))
    return stay, got, gate, mixed


def local(
    hidden_in,
    doc_ids,
    norm_gain,
    in_zx,
    in_bc,
    in_dt,
    conv_x,
    conv_bc,
    bias_x,
    bias_bc,
    dt_bias,
    a_log,
    d_skip,
    gated_gain,
    out_w,
):
    route = Route(tuple(lax.axis_size(a) for a in AXES))
    section = lax.axis_index("pipe")
    tp = lax.axis_index("tp")
    micro_count = hidden_in.shape[0]
    channels = gated_gain.shape[1]
    local_heads = dt_bias.shape[1]
    width = channels // local_heads
    depth = in_zx.shape[1]
    rows = doc_ids.shape[1]
    own_rows = hidden_in.shape[1]
    state_width = in_bc.shape[2] // 2
    heads = 8 if local_heads % 8 == 0 else local_heads
    tiles = local_heads // heads
    sizes = (rows, heads, width, tiles, state_width)
    full_width = channels * route.tps

    def lanes(a):
        return jnp.pad(a, ((0, 0), (0, LANES - local_heads)))

    w_zx = in_zx[0].reshape(depth, 2 * channels)
    small = jnp.concatenate([in_bc[0], lanes(in_dt[0])], 1)
    dtb = lanes(dt_bias)
    rate = lanes(-jnp.exp(a_log))
    skip = jnp.repeat(d_skip, width, axis=1)
    every = route.every()
    outputs = []
    for micro in range(micro_count):
        ids = doc_ids[micro].astype(f32)
        ids_row = jnp.broadcast_to(
            jnp.pad(ids[rows - 8 :], (0, depth - 8)).astype(bf16)[None, :], (HALO, depth)
        )
        current = hidden_in[micro]
        source = 0
        result = jnp.zeros_like(current)
        for pipe in range(route.pipes):
            if source == pipe:
                parts, halos = gather_rows(route, current, source, pipe, None, ids_row)
                before = sum(h[HALO, :8].astype(f32) for h in halos)
                before = jnp.where(lax.axis_index("seq") == 0, -1.0, before)
                idc = jnp.broadcast_to(
                    jnp.concatenate([before, ids])[:, None], (rows + 8, LANES)
                )
                idr = jnp.broadcast_to(ids[None, :], (8, rows))
            else:
                parts, halos = gather_rows(route, current, source, pipe)
            residual = parts[0]
            at = ((tp + jnp.arange(route.tps, dtype=jnp.int32)) % route.tps) * own_rows
            normed, x, xs, bc, acol, arow, ein, eall, states, sent = scan_call(
                at,
                parts,
                halos,
                norm_gain,
                small,
                w_zx,
                conv_x[0],
                conv_bc[0],
                bias_x,
                bias_bc,
                dtb,
                rate,
                idc,
                sizes,
            )
            stay, got, gate, y = exchange_states(
                route,
                sent,
                state_width,
                pipe,
                lambda: gate_call(normed, w_zx, sizes),
                lambda *a: inner_call(*a, bc, acol, arow, ein, states, skip, idc, idr, sizes),
                (x, xs),
            )
            swapped = lax.axis_index("seq") % 2
            total = None
            squares = None
            for distance in range(1, route.tps):
                at = jnp.stack([(tp + distance) % route.tps, swapped]).astype(jnp.int32)
                part, sq = out_call(
                    at, y, gate, bc, eall, stay, got, gated_gain, out_w[0], own_rows, sizes
                )
                pairs = [
                    ((pipe, s, t), (pipe, s, (t + distance) % route.tps)) for s, t in every
                ]
                part = route.move(part, pairs).astype(f32)
                sq = route.move(sq, pairs)
                total = part if total is None else total + part
                squares = sq if squares is None else squares + sq
            part, sq = out_call(
                jnp.stack([tp, swapped]).astype(jnp.int32),
                y, gate, bc, eall, stay, got, gated_gain, out_w[0], own_rows, sizes
            )
            total = part.astype(f32) if total is None else total + part.astype(f32)
            squares = sq if squares is None else squares + sq
            scale = lax.rsqrt(squares[:, 0:1] / full_width + epsilon)
            current = (residual.astype(f32) + scale * total).astype(bf16)
            source = pipe
            result = jnp.where(section == pipe, current, result)
        outputs.append(result)
    return jnp.stack(outputs)[None]


def solution(mesh):
    placed = (
        P(None, ("seq", "tp"), None),
        P(None, "seq"),
        P("pipe", None),
        P("pipe", None, None, "tp"),
        P("pipe", None, None),
        P("pipe", None, "tp"),
        P("pipe", None, "tp"),
        P("pipe", None, None),
        P("pipe", "tp"),
        P("pipe", None),
        P("pipe", "tp"),
        P("pipe", "tp"),
        P("pipe", "tp"),
        P("pipe", "tp"),
        P("pipe", "tp", None),
    )
    return jax.shard_map(
        local,
        mesh=mesh,
        in_specs=placed,
        out_specs=P("pipe", None, ("seq", "tp"), None),
        check_vma=False,
    )
```

```python
import functools

import jax
import jax.numpy as jnp
from jax import lax
from jax.experimental import pallas as pl
from jax.experimental.pallas import tpu as pltpu
from jax.sharding import PartitionSpec as P

AXES = ("pipe", "seq", "tp")
BLOCK = 256
HALO = 16
KEEP_ROWS = 16
CUTS = 4
LANES = 128
epsilon = 1e-05
highest = lax.Precision.HIGHEST
f32 = jnp.float32
bf16 = jnp.bfloat16


def dot(a, b):
    return jnp.dot(a, b, preferred_element_type=f32)


def cost(micros):
    return pl.CostEstimate(flops=int(micros * 2.5e8), bytes_accessed=0, transcendentals=0)


def silu(v):
    half = 0.5 * v
    return half + half * jnp.tanh(half)


def softplus(v):
    return jnp.maximum(v, 0.0) + jnp.log1p(jnp.exp(-jnp.abs(v)))


def spread_matrix(heads, width, tile):
    rows = lax.broadcasted_iota(jnp.int32, (LANES, heads * width), 0) - tile * heads
    cols = lax.broadcasted_iota(jnp.int32, (LANES, heads * width), 1)
    inside = (cols >= rows * width) & (cols < (rows + 1) * width)
    return jnp.where(inside, 1.0, 0.0).astype(bf16)


def weight_copies(source, held, sems, tile, first):
    depth, lanes = held.shape[1:]
    cut = depth // CUTS
    col = pl.multiple_of((first + tile) * lanes, LANES)
    return [
        pltpu.make_async_copy(
            source.at[pl.ds(k * cut, cut), pl.ds(col, lanes)],
            held.at[tile, pl.ds(k * cut, cut)],
            sems.at[tile, k],
        )
        for k in range(CUTS)
    ]


def conv_rows(raw_ref, keep_ref, taps, bias, start, stop, col):
    width = LANES
    out = bias + taps[3:4] * raw_ref[start + 8 : stop + 8, col : col + width]
    for tap in range(3):
        shifted_rows = raw_ref[start + 5 + tap : stop + 5 + tap, col : col + width]
        out = out + keep_ref[tap, start:stop] * (taps[tap : tap + 1] * shifted_rows)
    return silu(out)


def scan_kernel(rows, heads, width, shares, at_ref, *refs):
    part_refs, halo_refs = refs[:shares], refs[shares : 2 * shares]
    (
        gain_ref,
        small_ref,
        wx_ref,
        tapx_ref,
        tapbc_ref,
        biasx_ref,
        biasbc_ref,
        dtb_ref,
        rate_ref,
        idc_ref,
        normed_ref,
        x_ref,
        xs_ref,
        bc_ref,
        acol_ref,
        arow_ref,
        ein_ref,
        eall_ref,
        state_ref,
        sent_ref,
        raw,
        keep,
        stepc,
        wend,
        kept,
        lhs,
        held,
        sems,
        out_sem,
    ) = refs[2 * shares :]
    tiles = held.shape[0]
    step_at = pl.program_id(0)
    blocks = rows // BLOCK
    state_width = bc_ref.shape[1] // 2
    tile_lanes = heads * width
    unit = 256 if tile_lanes % 256 == 0 else LANES
    units = tile_lanes // unit

    saved = pltpu.make_async_copy(lhs, normed_ref, out_sem)

    @pl.when(step_at == 0)
    def _():
        for tile in range(tiles):
            for copy in weight_copies(wx_ref, held, sems, tile, tiles):
                copy.start()
        gain = gain_ref[...]

        def normalize(part):
            scale = lax.rsqrt(jnp.mean(part * part, axis=1, keepdims=True) + epsilon)
            return (part * scale * gain).astype(bf16)

        for share in range(shares):
            for begin in range(0, rows // shares, HALO):
                place = pl.multiple_of(at_ref[share] + begin, HALO)
                part = part_refs[share][begin : begin + HALO].astype(f32)
                lhs[pl.ds(place, HALO)] = normalize(part)
        halo = halo_refs[0][...].astype(f32)
        for other in halo_refs[1:]:
            halo = halo + other[...].astype(f32)
        lhs[rows:] = normalize(halo)
        saved.start()
        small = dot(lhs[...], small_ref[...])
        for tap in range(3):
            keep[tap] = (idc_ref[5 + tap : 5 + tap + rows] == idc_ref[8 : 8 + rows]).astype(f32)
        raw[0:8, 0 : 2 * state_width] = small[rows + HALO - 8 :, : 2 * state_width]
        raw[8 : 8 + rows, 0 : 2 * state_width] = small[:rows, : 2 * state_width]
        for col in range(0, 2 * state_width, LANES):
            bc_ref[:, col : col + LANES] = conv_rows(
                raw,
                keep,
                tapbc_ref[:, col : col + LANES],
                biasbc_ref[:, col : col + LANES],
                0,
                rows,
                col,
            ).astype(bf16)
        step = softplus(small[:rows, 2 * state_width :] + dtb_ref[...])
        log_step = step * rate_ref[...]
        at = lax.broadcasted_iota(jnp.int32, (BLOCK, BLOCK), 0)
        to = lax.broadcasted_iota(jnp.int32, (BLOCK, BLOCK), 1)
        lower = (at >= to).astype(f32)
        first_prev = idc_ref[7:8]
        before = jnp.zeros((1, LANES), f32)
        kept[...] = jnp.zeros_like(kept)
        for block in range(blocks):
            r0, r1 = block * BLOCK, (block + 1) * BLOCK
            ids = idc_ref[8 + r0 : 8 + r1]
            prev = idc_ref[7 + r0 : 8 + r0]
            last = idc_ref[7 + r1 : 8 + r1]
            part_step = step[r0:r1]
            total = jnp.dot(lower, log_step[r0:r1], precision=highest, preferred_element_type=f32)
            end = total[BLOCK - 1 : BLOCK]
            acol_ref[r0:r1] = total
            arow_ref[:, r0:r1] = total.T
            ein_ref[r0:r1] = (jnp.exp(total) * (ids == prev).astype(f32)).astype(bf16)
            eall_ref[r0:r1] = (jnp.exp(total + before) * (ids == first_prev).astype(f32)).astype(
                bf16
            )
            stepc[r0:r1] = part_step.astype(bf16)
            wend[r0:r1] = (jnp.exp(end - total) * (ids == last).astype(f32) * part_step).astype(
                bf16
            )
            kept[block : block + 1] = jnp.exp(end) * (last == prev).astype(f32)
            before = before + end
        kept[blocks : blocks + 1] = jnp.exp(before) * (
            idc_ref[7 + rows : 8 + rows] == first_prev
        ).astype(f32)

    spread = spread_matrix(heads, width, step_at)
    kept_now = kept[...]
    high = kept_now.astype(bf16)
    low = (kept_now - high.astype(f32)).astype(bf16)
    keep_lanes = dot(high, spread) + dot(low, spread)
    step_lanes = dot(stepc[...], spread)
    wend_lanes = dot(wend[...], spread)
    for copy in weight_copies(wx_ref, held, sems, step_at, tiles):
        copy.wait()
    for u in range(units):
        cols = slice(u * unit, (u + 1) * unit)
        fresh = dot(lhs[...], held[step_at, :, cols])
        raw[0:8, cols] = fresh[rows + HALO - 8 :]
        raw[8 : 8 + rows, cols] = fresh[:rows]
    at = lax.broadcasted_iota(jnp.int32, (KEEP_ROWS, unit), 0)
    for u in range(units):
        cols = slice(u * unit, (u + 1) * unit)
        running = None
        for block in range(blocks):
            r0, r1 = block * BLOCK, (block + 1) * BLOCK
            pieces = []
            for col in range(u * unit, (u + 1) * unit, LANES):
                x_now = conv_rows(
                    raw,
                    keep,
                    tapx_ref[:, col : col + LANES],
                    biasx_ref[:, col : col + LANES],
                    r0,
                    r1,
                    col,
                )
                x_ref[r0:r1, col : col + LANES] = x_now.astype(bf16)
                xs_ref[r0:r1, col : col + LANES] = (
                    x_now * step_lanes[r0:r1, col : col + LANES]
                ).astype(bf16)
                pieces.append((x_now * wend_lanes[r0:r1, col : col + LANES]).astype(bf16))
            local = lax.dot_general(
                bc_ref[r0:r1, 0:state_width],
                jnp.concatenate(pieces, 1),
                (((0,), (0,)), ((), ())),
                preferred_element_type=f32,
            )
            if running is not None:
                local = local + keep_lanes[block : block + 1, cols] * running
            running = local
            if block < blocks - 1:
                state_ref[block, :, cols] = running.astype(bf16)
        sent_ref[0:state_width, cols] = running.astype(bf16)
        shard_row = keep_lanes[blocks : blocks + 1, cols]
        shard_high = shard_row.astype(bf16).astype(f32)
        both = jnp.where(
            at == 0, shard_high, jnp.where(at == 1, shard_row - shard_high, 0.0)
        )
        sent_ref[state_width:, cols] = both.astype(bf16)

    @pl.when(step_at == tiles - 1)
    def _():
        saved.wait()


def scan_call(at, parts, halos, gain, small, w_zx, tapx, tapbc, biasx, biasbc, dtb, rate, idc, sizes):
    rows, heads, width, tiles, state_width = sizes
    shares, depth = len(parts), w_zx.shape[0]
    tile_lanes = heads * width
    channels = tiles * tile_lanes
    blocks = rows // BLOCK

    def whole(*shape):
        return pl.BlockSpec(shape, lambda i, at: (0,) * len(shape))

    def column(lead):
        return pl.BlockSpec((lead, tile_lanes), lambda i, at: (0, i))

    return pl.pallas_call(
        functools.partial(scan_kernel, rows, heads, width, shares),
        grid_spec=pltpu.PrefetchScalarGridSpec(
            num_scalar_prefetch=1,
            grid=(tiles,),
            in_specs=[whole(rows // shares, depth)] * shares
            + [whole(HALO, depth)] * shares
            + [
                whole(1, depth),
                whole(depth, 2 * state_width + LANES),
                pl.BlockSpec(memory_space=pltpu.HBM),
                column(4),
                whole(4, 2 * state_width),
                column(1),
                whole(1, 2 * state_width),
                whole(1, LANES),
                whole(1, LANES),
                whole(rows + 8, LANES),
            ],
            out_specs=[
                pl.BlockSpec(memory_space=pltpu.HBM),
                column(rows),
                column(rows),
                whole(rows, 2 * state_width),
                whole(rows, LANES),
                whole(LANES, rows),
                whole(rows, LANES),
                whole(rows, LANES),
                pl.BlockSpec(
                    (max(blocks - 1, 1), state_width, tile_lanes), lambda i, at: (0, 0, i)
                ),
                column(state_width + KEEP_ROWS),
            ],
            scratch_shapes=[
                pltpu.VMEM((rows + 8, max(tile_lanes, 2 * state_width)), f32),
                pltpu.VMEM((3, rows, LANES), f32),
                pltpu.VMEM((rows, LANES), bf16),
                pltpu.VMEM((rows, LANES), bf16),
                pltpu.VMEM((max(8, blocks + 1), LANES), f32),
                pltpu.VMEM((rows + HALO, depth), bf16),
                pltpu.VMEM((tiles, depth, tile_lanes), bf16),
                pltpu.SemaphoreType.DMA((tiles, CUTS)),
                pltpu.SemaphoreType.DMA,
            ],
        ),
        out_shape=[
            jax.ShapeDtypeStruct((rows + HALO, depth), bf16),
            jax.ShapeDtypeStruct((rows, channels), bf16),
            jax.ShapeDtypeStruct((rows, channels), bf16),
            jax.ShapeDtypeStruct((rows, 2 * state_width), bf16),
            jax.ShapeDtypeStruct((rows, LANES), f32),
            jax.ShapeDtypeStruct((LANES, rows), f32),
            jax.ShapeDtypeStruct((rows, LANES), bf16),
            jax.ShapeDtypeStruct((rows, LANES), bf16),
            jax.ShapeDtypeStruct((max(blocks - 1, 1), state_width, channels), bf16),
            jax.ShapeDtypeStruct((state_width + KEEP_ROWS, channels), bf16),
        ],
        compiler_params=pltpu.CompilerParams(
            dimension_semantics=("arbitrary",), vmem_limit_bytes=60 * 2**20
        ),
        cost_estimate=cost(15),
        name="scan",
    )(at, *parts, *halos, gain, small, w_zx, tapx, tapbc, biasx, biasbc, dtb, rate, idc)


def inner_kernel(
    rows,
    heads,
    width,
    x_ref,
    xs_ref,
    bc_ref,
    acol_ref,
    arow_ref,
    ein_ref,
    state_ref,
    skip_ref,
    idc_ref,
    idr_ref,
    y_ref,
    gram,
):
    blocks = rows // BLOCK
    state_width = bc_ref.shape[1] // 2

    @pl.when(pl.program_id(0) == 0)
    def _():
        at = lax.broadcasted_iota(jnp.int32, (BLOCK, BLOCK), 0)
        to = lax.broadcasted_iota(jnp.int32, (BLOCK, BLOCK), 1)
        for block in range(blocks):
            r0, r1 = block * BLOCK, (block + 1) * BLOCK
            b_rows = bc_ref[r0:r1, 0:state_width]
            c_rows = bc_ref[r0:r1, state_width:]
            ids = jnp.concatenate([idc_ref[8 + r0 : 8 + r1]] * (BLOCK // LANES), 1)
            same = (at >= to) & (ids == idr_ref[0:1, r0:r1])
            product = lax.dot_general(
                c_rows, b_rows, (((1,), (1,)), ((), ())), preferred_element_type=f32
            )
            gram[block] = jnp.where(same, product, 0.0)

    tile = pl.program_id(0)
    spread = spread_matrix(heads, width, tile)
    acol = pltpu.roll(acol_ref[...], lax.rem(LANES - tile * heads, LANES), 1)
    lane = lax.broadcasted_iota(jnp.int32, (BLOCK, LANES), 1)
    pack = LANES // width
    for block in range(blocks):
        r0, r1 = block * BLOCK, (block + 1) * BLOCK
        if block > 0:
            carried = dot(bc_ref[r0:r1, state_width:], state_ref[block - 1])
            carried = carried * dot(ein_ref[r0:r1], spread)
        for first in range(0, heads, pack):
            cols = slice(first * width, (first + pack) * width)
            xs_now = xs_ref[r0:r1, cols]
            total = None
            for inner in range(pack):
                head = first + inner
                gap = acol[r0:r1, head : head + 1] - arow_ref[head : head + 1, r0:r1]
                mix = (jnp.exp(jnp.minimum(gap, 0.0)) * gram[block]).astype(bf16)
                part = dot(mix, xs_now)
                total = part if total is None else jnp.where(lane < inner * width, total, part)
            total = total + skip_ref[:, cols] * x_ref[r0:r1, cols].astype(f32)
            if block > 0:
                total = total + carried[:, cols]
            y_ref[r0:r1, cols] = total.astype(bf16)


def inner_call(x, xs, bc, acol, arow, ein, states, skip, idc, idr, sizes):
    rows, heads, width, tiles, state_width = sizes
    tile_lanes = heads * width
    channels = tiles * tile_lanes
    blocks = rows // BLOCK

    def whole(*shape):
        return pl.BlockSpec(shape, lambda i: (0,) * len(shape))

    def column(lead):
        return pl.BlockSpec((lead, tile_lanes), lambda i: (0, i))

    arow_rows = heads if heads % 8 == 0 else LANES

    return pl.pallas_call(
        functools.partial(inner_kernel, rows, heads, width),
        grid=(tiles,),
        in_specs=[
            column(rows),
            column(rows),
            whole(rows, 2 * state_width),
            whole(rows, LANES),
            pl.BlockSpec((arow_rows, rows), lambda i: (i, 0)),
            whole(rows, LANES),
            pl.BlockSpec((max(blocks - 1, 1), state_width, tile_lanes), lambda i: (0, 0, i)),
            column(1),
            whole(rows + 8, LANES),
            whole(8, rows),
        ],
        out_specs=column(rows),
        out_shape=jax.ShapeDtypeStruct((rows, channels), bf16),
        scratch_shapes=[pltpu.VMEM((blocks, BLOCK, BLOCK), f32)],
        compiler_params=pltpu.CompilerParams(
            dimension_semantics=("arbitrary",), vmem_limit_bytes=60 * 2**20
        ),
        cost_estimate=cost(11),
        name="inner",
    )(x, xs, bc, acol, arow, ein, states, skip, idc, idr)


def gate_kernel(normed_ref, wz_ref, gate_ref, lhs, held, sems, row_sems):
    tile = pl.program_id(0)
    rows = lhs.shape[0]
    cut = rows // CUTS
    loads = [
        pltpu.make_async_copy(
            normed_ref.at[pl.ds(k * cut, cut)], lhs.at[pl.ds(k * cut, cut)], row_sems.at[k]
        )
        for k in range(CUTS)
    ]

    @pl.when(tile == 0)
    def _():
        for copy in loads:
            copy.start()
        for other in range(held.shape[0]):
            for copy in weight_copies(wz_ref, held, sems, other, 0):
                copy.start()
        for copy in loads:
            copy.wait()

    for copy in weight_copies(wz_ref, held, sems, tile, 0):
        copy.wait()
    gate_ref[...] = silu(dot(lhs[...], held[tile])).astype(bf16)


def gate_call(normed, w_zx, sizes):
    rows, heads, width, tiles, _ = sizes
    depth = normed.shape[1]
    tile_lanes = heads * width
    return pl.pallas_call(
        gate_kernel,
        grid=(tiles,),
        in_specs=[pl.BlockSpec(memory_space=pltpu.HBM)] * 2,
        out_specs=pl.BlockSpec((rows, tile_lanes), lambda i: (0, i)),
        scratch_shapes=[
            pltpu.VMEM((rows, depth), bf16),
            pltpu.VMEM((tiles, depth, tile_lanes), bf16),
            pltpu.SemaphoreType.DMA((tiles, CUTS)),
            pltpu.SemaphoreType.DMA((CUTS,)),
        ],
        out_shape=jax.ShapeDtypeStruct((rows, tiles * tile_lanes), bf16),
        compiler_params=pltpu.CompilerParams(
            dimension_semantics=("arbitrary",), vmem_limit_bytes=60 * 2**20
        ),
        cost_estimate=cost(8),
        name="gate",
    )(normed, w_zx)


def out_kernel(
    heads,
    width,
    tiles,
    at_ref,
    y_ref,
    gate_ref,
    bc_ref,
    eall_ref,
    stay_ref,
    got_ref,
    gain_ref,
    w_ref,
    p_ref,
    sq_ref,
    lhs,
    coming,
    y_held,
    gate_held,
    held,
    sems,
    row_sems,
):
    state_width = bc_ref.shape[1] // 2
    tile_lanes = heads * width
    half = stay_ref.shape[1]
    piece = pl.program_id(0)
    count = lhs.shape[0]
    mine = pl.ds(pl.multiple_of(at_ref[0] * count, count), count)
    loads = [
        pltpu.make_async_copy(y_ref.at[mine], y_held, row_sems.at[0]),
        pltpu.make_async_copy(gate_ref.at[mine], gate_held, row_sems.at[1]),
    ]

    @pl.when(piece == 0)
    def _():
        for copy in loads:
            copy.start()
        for other in range(held.shape[0]):
            for copy in weight_copies(w_ref, held, sems, other, 0):
                copy.start()
        for copy in loads:
            copy.wait()
        swapped = at_ref[1] != 0
        coming[:, :half] = jnp.where(swapped, got_ref[...], stay_ref[...])
        coming[:, half:] = jnp.where(swapped, stay_ref[...], got_ref[...])
        squares = None
        for tile in range(tiles):
            cols = slice(tile * tile_lanes, (tile + 1) * tile_lanes)
            carried = dot(bc_ref[:, state_width:], coming[:, cols])
            carried = carried * dot(eall_ref[...], spread_matrix(heads, width, tile))
            gated = (y_held[:, cols].astype(f32) + carried) * gate_held[:, cols].astype(f32)
            part = jnp.sum(gated * gated, axis=1, keepdims=True)
            squares = part if squares is None else squares + part
            lhs[:, cols] = (gated * gain_ref[:, cols]).astype(bf16)
        sq_ref[...] = jnp.broadcast_to(squares, sq_ref.shape)

    for copy in weight_copies(w_ref, held, sems, piece, 0):
        copy.wait()
    p_ref[...] = dot(lhs[...], held[piece]).astype(bf16)


def out_call(at, y, gate, bc, eall, stay, got, gain, w_out, count, sizes):
    rows, heads, width, tiles, state_width = sizes
    channels, depth = w_out.shape
    piece = 512 if depth % 512 == 0 else depth

    def taken(lanes):
        return pl.BlockSpec((count, lanes), lambda i, at: (at[0], 0))

    def whole(*shape):
        return pl.BlockSpec(shape, lambda i, at: (0,) * len(shape))

    return pl.pallas_call(
        functools.partial(out_kernel, heads, width, tiles),
        grid_spec=pltpu.PrefetchScalarGridSpec(
            num_scalar_prefetch=1,
            grid=(depth // piece,),
            in_specs=[
                pl.BlockSpec(memory_space=pltpu.HBM),
                pl.BlockSpec(memory_space=pltpu.HBM),
                taken(2 * state_width),
                taken(LANES),
                whole(state_width, channels // 2),
                whole(state_width, channels // 2),
                whole(1, channels),
                pl.BlockSpec(memory_space=pltpu.HBM),
            ],
            out_specs=[
                pl.BlockSpec((count, piece), lambda i, at: (0, i)),
                whole(count, LANES),
            ],
            scratch_shapes=[
                pltpu.VMEM((count, channels), bf16),
                pltpu.VMEM((state_width, channels), bf16),
                pltpu.VMEM((count, channels), bf16),
                pltpu.VMEM((count, channels), bf16),
                pltpu.VMEM((depth // piece, channels, piece), bf16),
                pltpu.SemaphoreType.DMA((depth // piece, CUTS)),
                pltpu.SemaphoreType.DMA((2,)),
            ],
        ),
        out_shape=[
            jax.ShapeDtypeStruct((count, depth), bf16),
            jax.ShapeDtypeStruct((count, LANES), f32),
        ],
        compiler_params=pltpu.CompilerParams(
            dimension_semantics=("arbitrary",), vmem_limit_bytes=60 * 2**20
        ),
        cost_estimate=cost(6),
        name="outp",
    )(at, y, gate, bc, eall, stay, got, gain, w_out)


class Route:
    def __init__(self, sizes):
        self.pipes, self.seqs, self.tps = sizes

    def spot(self, pipe, seq, tp):
        return (pipe * self.seqs + seq) * self.tps + tp

    def move(self, block, pairs):
        return lax.ppermute(
            block, AXES, [(self.spot(*source), self.spot(*target)) for source, target in pairs]
        )

    def every(self):
        return [(s, t) for s in range(self.seqs) for t in range(self.tps)]


def gather_rows(route, own, source_pipe, pipe, tail_after=None, ids_row=None):
    tps, seqs = route.tps, route.seqs
    parts = [own]
    if source_pipe != pipe:
        parts = [route.move(own, [((source_pipe, s, t), (pipe, s, t)) for s, t in route.every()])]
    for distance in range(1, tps):
        parts.append(
            route.move(
                own,
                [
                    ((source_pipe, s, (t + distance) % tps), (pipe, s, t))
                    for s, t in route.every()
                ],
            )
        )
    tail = own[own.shape[0] - HALO :]
    if ids_row is not None:
        tail = jnp.concatenate([tail, ids_row], 0)
    pipes = [(source_pipe, pipe)] if ids_row is None else [(p, p) for p in range(route.pipes)]
    halos = [
        route.move(
            tail,
            [((a, s, tps - 1), (b, s + 1, t)) for a, b in pipes for s in range(seqs - 1)],
        )
        for t in range(tps)
    ]
    return parts, halos


def exchange_states(route, sent, state_width, pipe, under_swap, under_scan, scan_inputs):
    seqs = route.seqs
    outer, side = seqs // 2, lax.axis_index("seq") % 2
    half = sent.shape[1] // 2
    is_first = side == 0

    def swap(block):
        return route.move(
            block, [((pipe, s, t), (pipe, s + 1 - 2 * (s % 2), t)) for s, t in route.every()]
        )

    def parted(block):
        block = block.astype(f32)
        keep = block[state_width : state_width + 1] + block[state_width + 1 : state_width + 2]
        return block[:state_width], keep

    def joined(state, keep):
        high = keep.astype(bf16)
        low = (keep - high.astype(f32)).astype(bf16)
        rest = jnp.zeros((KEEP_ROWS - 2, half), bf16)
        return jnp.concatenate([state.astype(bf16), high, low, rest], 0)

    low, high = sent[:, :half], sent[:, half:]
    mine = jnp.where(is_first, low, high)
    theirs = swap(jnp.where(is_first, high, low))
    theirs, gate = lax.optimization_barrier((theirs, under_swap()))
    early, keep_early = parted(jnp.where(is_first, mine, theirs))
    late, keep_late = parted(jnp.where(is_first, theirs, mine))
    pair = joined(keep_late * early + late, keep_early * keep_late)
    pair, scan_inputs = lax.optimization_barrier((pair, scan_inputs))
    arrivals = []
    for distance in range(1, outer):
        pairs = [
            ((pipe, s - 2 * distance, t), (pipe, s, t))
            for s, t in route.every()
            if s - 2 * distance >= 0
        ]
        arrivals.append(route.move(pair, pairs))
    arrivals, mixed = lax.optimization_barrier((arrivals, under_scan(*scan_inputs)))
    total, weight = parted(arrivals[0])
    for came in arrivals[1:]:
        came, keep_came = parted(came)
        total = total + weight * came
        weight = weight * keep_came
    after_early = keep_early * total + early
    stay = jnp.where(is_first, total, after_early).astype(bf16)
    got = swap(jnp.where(is_first, after_early, total).astype(bf16))
    return stay, got, gate, mixed


def local(
    hidden_in,
    doc_ids,
    norm_gain,
    in_zx,
    in_bc,
    in_dt,
    conv_x,
    conv_bc,
    bias_x,
    bias_bc,
    dt_bias,
    a_log,
    d_skip,
    gated_gain,
    out_w,
):
    route = Route(tuple(lax.axis_size(a) for a in AXES))
    section = lax.axis_index("pipe")
    tp = lax.axis_index("tp")
    micro_count = hidden_in.shape[0]
    channels = gated_gain.shape[1]
    local_heads = dt_bias.shape[1]
    width = channels // local_heads
    depth = in_zx.shape[1]
    rows = doc_ids.shape[1]
    own_rows = hidden_in.shape[1]
    state_width = in_bc.shape[2] // 2
    heads = 8 if local_heads % 8 == 0 else local_heads
    tiles = local_heads // heads
    sizes = (rows, heads, width, tiles, state_width)
    full_width = channels * route.tps

    def lanes(a):
        return jnp.pad(a, ((0, 0), (0, LANES - local_heads)))

    w_zx = in_zx[0].reshape(depth, 2 * channels)
    small = jnp.concatenate([in_bc[0], lanes(in_dt[0])], 1)
    dtb = lanes(dt_bias)
    rate = lanes(-jnp.exp(a_log))
    skip = jnp.repeat(d_skip, width, axis=1)
    every = route.every()
    outputs = []
    for micro in range(micro_count):
        ids = doc_ids[micro].astype(f32)
        ids_row = jnp.broadcast_to(
            jnp.pad(ids[rows - 8 :], (0, depth - 8)).astype(bf16)[None, :], (HALO, depth)
        )
        current = hidden_in[micro]
        source = 0
        result = jnp.zeros_like(current)
        for pipe in range(route.pipes):
            if source == pipe:
                parts, halos = gather_rows(route, current, source, pipe, None, ids_row)
                before = sum(h[HALO, :8].astype(f32) for h in halos)
                before = jnp.where(lax.axis_index("seq") == 0, -1.0, before)
                idc = jnp.broadcast_to(
                    jnp.concatenate([before, ids])[:, None], (rows + 8, LANES)
                )
                idr = jnp.broadcast_to(ids[None, :], (8, rows))
            else:
                parts, halos = gather_rows(route, current, source, pipe)
            residual = parts[0]
            at = ((tp + jnp.arange(route.tps, dtype=jnp.int32)) % route.tps) * own_rows
            normed, x, xs, bc, acol, arow, ein, eall, states, sent = scan_call(
                at,
                parts,
                halos,
                norm_gain,
                small,
                w_zx,
                conv_x[0],
                conv_bc[0],
                bias_x,
                bias_bc,
                dtb,
                rate,
                idc,
                sizes,
            )
            stay, got, gate, y = exchange_states(
                route,
                sent,
                state_width,
                pipe,
                lambda: gate_call(normed, w_zx, sizes),
                lambda *a: inner_call(*a, bc, acol, arow, ein, states, skip, idc, idr, sizes),
                (x, xs),
            )
            swapped = lax.axis_index("seq") % 2
            total = None
            squares = None
            for distance in range(1, route.tps):
                at = jnp.stack([(tp + distance) % route.tps, swapped]).astype(jnp.int32)
                part, sq = out_call(
                    at, y, gate, bc, eall, stay, got, gated_gain, out_w[0], own_rows, sizes
                )
                pairs = [
                    ((pipe, s, t), (pipe, s, (t + distance) % route.tps)) for s, t in every
                ]
                part = route.move(part, pairs).astype(f32)
                sq = route.move(sq, pairs)
                total = part if total is None else total + part
                squares = sq if squares is None else squares + sq
            part, sq = out_call(
                jnp.stack([tp, swapped]).astype(jnp.int32),
                y, gate, bc, eall, stay, got, gated_gain, out_w[0], own_rows, sizes
            )
            total = part.astype(f32) if total is None else total + part.astype(f32)
            squares = sq if squares is None else squares + sq
            scale = lax.rsqrt(squares[:, 0:1] / full_width + epsilon)
            current = (residual.astype(f32) + scale * total).astype(bf16)
            source = pipe
            result = jnp.where(section == pipe, current, result)
        outputs.append(result)
    return jnp.stack(outputs)[None]


def solution(mesh):
    placed = (
        P(None, ("seq", "tp"), None),
        P(None, "seq"),
        P("pipe", None),
        P("pipe", None, None, "tp"),
        P("pipe", None, None),
        P("pipe", None, "tp"),
        P("pipe", None, "tp"),
        P("pipe", None, None),
        P("pipe", "tp"),
        P("pipe", None),
        P("pipe", "tp"),
        P("pipe", "tp"),
        P("pipe", "tp"),
        P("pipe", "tp"),
        P("pipe", "tp", None),
    )
    return jax.shard_map(
        local,
        mesh=mesh,
        in_specs=placed,
        out_specs=P("pipe", None, ("seq", "tp"), None),
        check_vma=False,
    )
```

```python
import functools

import jax
import jax.numpy as jnp
from jax import lax
from jax.experimental import pallas as pl
from jax.experimental.pallas import tpu as pltpu
from jax.sharding import PartitionSpec as P

AXES = ("pipe", "seq", "tp")
BLOCK = 256
HALO = 16
KEEP_ROWS = 16
SLOTS = 3
STRIP = 64
LANES = 128
epsilon = 1e-05
highest = lax.Precision.HIGHEST
f32 = jnp.float32
bf16 = jnp.bfloat16


def dot(a, b):
    return jnp.dot(a, b, preferred_element_type=f32)


def cost(micros):
    return pl.CostEstimate(flops=int(micros * 2.5e8), bytes_accessed=0, transcendentals=0)


def silu(v):
    half = 0.5 * v
    return half + half * jnp.tanh(half)


def softplus(v):
    return jnp.maximum(v, 0.0) + jnp.log1p(jnp.exp(-jnp.abs(v)))


def spread_matrix(heads, width, tile):
    rows = lax.broadcasted_iota(jnp.int32, (LANES, heads * width), 0) - tile * heads
    cols = lax.broadcasted_iota(jnp.int32, (LANES, heads * width), 1)
    inside = (cols >= rows * width) & (cols < (rows + 1) * width)
    return jnp.where(inside, 1.0, 0.0).astype(bf16)


def stream(step_at, count, source, held, sems, place, meanwhile=None):
    slots = held.shape[0]

    def copy(tile):
        slot = lax.rem(tile, slots)
        return pltpu.make_async_copy(source.at[place(tile)], held.at[slot], sems.at[slot])

    @pl.when(step_at == 0)
    def _():
        for tile in range(min(slots - 1, count)):
            copy(tile).start()
        if meanwhile is not None:
            meanwhile()

    if count >= slots:

        @pl.when(step_at + slots - 1 < count)
        def _():
            copy(step_at + slots - 1).start()

    copy(step_at).wait()
    return held.at[lax.rem(step_at, slots)]


def column_tile(depth, lanes, first):
    return lambda tile: (
        pl.ds(0, depth),
        pl.ds(pl.multiple_of(first + tile * lanes, LANES), lanes),
    )


def conv_rows(raw_ref, keep_ref, taps, bias, start, stop, col):
    width = LANES
    out = bias + taps[3:4] * raw_ref[start + 8 : stop + 8, col : col + width]
    for tap in range(3):
        shifted_rows = raw_ref[start + 5 + tap : stop + 5 + tap, col : col + width]
        out = out + keep_ref[tap, start:stop] * (taps[tap : tap + 1] * shifted_rows)
    return silu(out)


def scan_kernel(rows, heads, width, shares, at_ref, *refs):
    part_refs, halo_refs = refs[:shares], refs[shares : 2 * shares]
    (
        gain_ref,
        wbc_ref,
        wdt_ref,
        wx_ref,
        tapx_ref,
        tapbc_ref,
        biasx_ref,
        biasbc_ref,
        dtb_ref,
        rate_ref,
        idc_ref,
        normed_ref,
        x_ref,
        xs_ref,
        bc_ref,
        acol_ref,
        arow_ref,
        ein_ref,
        eall_ref,
        state_ref,
        sent_ref,
        raw,
        keep,
        stepc,
        wend,
        kept,
        lhs,
        weighted,
        step_lanes,
        wend_lanes,
        held,
        sems,
        out_sem,
    ) = refs[2 * shares :]
    step_at = pl.program_id(0)
    blocks = rows // BLOCK
    state_width = bc_ref.shape[1] // 2
    tile_lanes = heads * width
    unit = 256 if tile_lanes % 256 == 0 else LANES
    units = tile_lanes // unit

    saved = pltpu.make_async_copy(lhs, normed_ref, out_sem)

    @pl.when(step_at == 0)
    def _():
        gain = gain_ref[...]

        def normalize(part):
            scale = lax.rsqrt(jnp.mean(part * part, axis=1, keepdims=True) + epsilon)
            return (part * scale * gain).astype(bf16)

        for share in range(shares):
            for begin in range(0, rows // shares, HALO):
                place = pl.multiple_of(at_ref[share] + begin, HALO)
                part = part_refs[share][begin : begin + HALO].astype(f32)
                lhs[pl.ds(place, HALO)] = normalize(part)
        halo = halo_refs[0][...].astype(f32)
        for other in halo_refs[1:]:
            halo = halo + other[...].astype(f32)
        lhs[rows:] = normalize(halo)
        saved.start()
        small = dot(lhs[...], wbc_ref[...])
        dt_raw = lax.dot_general(
            lhs[0:rows], wdt_ref[...], (((1,), (1,)), ((), ())), preferred_element_type=f32
        )
        for tap in range(3):
            keep[tap] = (idc_ref[5 + tap : 5 + tap + rows] == idc_ref[8 : 8 + rows]).astype(f32)
        raw[0:8, 0 : 2 * state_width] = small[rows + HALO - 8 :]
        raw[8 : 8 + rows, 0 : 2 * state_width] = small[:rows]
        for col in range(0, 2 * state_width, LANES):
            strip_cols = slice(col, col + LANES)
            for a in range(0, rows, STRIP):
                bc_ref[a : a + STRIP, strip_cols] = conv_rows(
                    raw,
                    keep,
                    tapbc_ref[:, strip_cols],
                    biasbc_ref[:, strip_cols],
                    a,
                    a + STRIP,
                    col,
                ).astype(bf16)
        step = softplus(dt_raw + dtb_ref[...])
        log_step = step * rate_ref[...]
        at = lax.broadcasted_iota(jnp.int32, (BLOCK, BLOCK), 0)
        to = lax.broadcasted_iota(jnp.int32, (BLOCK, BLOCK), 1)
        lower = (at >= to).astype(f32)
        first_prev = idc_ref[7:8]
        before = jnp.zeros((1, LANES), f32)
        kept[...] = jnp.zeros_like(kept)
        for block in range(blocks):
            r0, r1 = block * BLOCK, (block + 1) * BLOCK
            ids = idc_ref[8 + r0 : 8 + r1]
            prev = idc_ref[7 + r0 : 8 + r0]
            last = idc_ref[7 + r1 : 8 + r1]
            part_step = step[r0:r1]
            total = jnp.dot(lower, log_step[r0:r1], precision=highest, preferred_element_type=f32)
            end = total[BLOCK - 1 : BLOCK]
            acol_ref[r0:r1] = total
            arow_ref[:, r0:r1] = total.T
            ein_ref[r0:r1] = (jnp.exp(total) * (ids == prev).astype(f32)).astype(bf16)
            eall_ref[r0:r1] = (jnp.exp(total + before) * (ids == first_prev).astype(f32)).astype(
                bf16
            )
            stepc[r0:r1] = part_step.astype(bf16)
            wend[r0:r1] = (jnp.exp(end - total) * (ids == last).astype(f32) * part_step).astype(
                bf16
            )
            kept[block : block + 1] = jnp.exp(end) * (last == prev).astype(f32)
            before = before + end
        kept[blocks : blocks + 1] = jnp.exp(before) * (
            idc_ref[7 + rows : 8 + rows] == first_prev
        ).astype(f32)

    spread = spread_matrix(heads, width, step_at)
    kept_now = kept[...]
    high = kept_now.astype(bf16)
    low = (kept_now - high.astype(f32)).astype(bf16)
    keep_lanes = dot(high, spread) + dot(low, spread)
    step_lanes[...] = dot(stepc[...], spread)
    wend_lanes[...] = dot(wend[...], spread)
    tiles = wx_ref.shape[1] // (2 * tile_lanes)
    depth = wx_ref.shape[0]
    weights = stream(
        step_at, tiles, wx_ref, held, sems, column_tile(depth, tile_lanes, tiles * tile_lanes)
    )
    for u in range(units):
        cols = slice(u * unit, (u + 1) * unit)
        fresh = dot(lhs[...], weights[:, cols])
        raw[0:8, cols] = fresh[rows + HALO - 8 :]
        raw[8 : 8 + rows, cols] = fresh[:rows]
    at = lax.broadcasted_iota(jnp.int32, (KEEP_ROWS, unit), 0)
    for u in range(units):
        cols = slice(u * unit, (u + 1) * unit)
        running = None
        for block in range(blocks):
            r0, r1 = block * BLOCK, (block + 1) * BLOCK
            for col in range(u * unit, (u + 1) * unit, LANES):
                strip_cols = slice(col, col + LANES)
                taps = tapx_ref[:, strip_cols]
                bias = biasx_ref[:, strip_cols]
                for a in range(r0, r1, STRIP):
                    b = a + STRIP
                    x_now = conv_rows(raw, keep, taps, bias, a, b, col)
                    x_ref[a:b, strip_cols] = x_now.astype(bf16)
                    xs_ref[a:b, strip_cols] = (x_now * step_lanes[a:b, strip_cols]).astype(bf16)
                    weighted[a:b, strip_cols] = (x_now * wend_lanes[a:b, strip_cols]).astype(bf16)
            local = lax.dot_general(
                bc_ref[r0:r1, 0:state_width],
                weighted[r0:r1, cols],
                (((0,), (0,)), ((), ())),
                preferred_element_type=f32,
            )
            if running is not None:
                local = local + keep_lanes[block : block + 1, cols] * running
            running = local
            if block < blocks - 1:
                state_ref[block, :, cols] = running.astype(bf16)
        sent_ref[0:state_width, cols] = running.astype(bf16)
        shard_row = keep_lanes[blocks : blocks + 1, cols]
        shard_high = shard_row.astype(bf16).astype(f32)
        both = jnp.where(
            at == 0, shard_high, jnp.where(at == 1, shard_row - shard_high, 0.0)
        )
        sent_ref[state_width:, cols] = both.astype(bf16)

    @pl.when(step_at == pl.num_programs(0) - 1)
    def _():
        saved.wait()


def scan_call(at, parts, halos, gain, wbc, wdt, w_zx, tapx, tapbc, biasx, biasbc, dtb, rate, idc, sizes):
    rows, heads, width, tiles, state_width = sizes
    shares, depth = len(parts), w_zx.shape[0]
    tile_lanes = heads * width
    channels = tiles * tile_lanes
    blocks = rows // BLOCK

    def whole(*shape):
        return pl.BlockSpec(shape, lambda i, at: (0,) * len(shape))

    def column(lead):
        return pl.BlockSpec((lead, tile_lanes), lambda i, at: (0, i))

    return pl.pallas_call(
        functools.partial(scan_kernel, rows, heads, width, shares),
        grid_spec=pltpu.PrefetchScalarGridSpec(
            num_scalar_prefetch=1,
            grid=(tiles,),
            in_specs=[whole(rows // shares, depth)] * shares
            + [whole(HALO, depth)] * shares
            + [
                whole(1, depth),
                whole(depth, 2 * state_width),
                whole(LANES, depth),
                pl.BlockSpec(memory_space=pltpu.HBM),
                column(4),
                whole(4, 2 * state_width),
                column(1),
                whole(1, 2 * state_width),
                whole(1, LANES),
                whole(1, LANES),
                whole(rows + 8, LANES),
            ],
            out_specs=[
                pl.BlockSpec(memory_space=pltpu.HBM),
                pl.BlockSpec((None, rows, tile_lanes), lambda i, at: (i, 0, 0)),
                pl.BlockSpec((None, rows, tile_lanes), lambda i, at: (i, 0, 0)),
                whole(rows, 2 * state_width),
                whole(rows, LANES),
                whole(LANES, rows),
                whole(rows, LANES),
                whole(rows, LANES),
                pl.BlockSpec(
                    (max(blocks - 1, 1), state_width, tile_lanes), lambda i, at: (0, 0, i)
                ),
                column(state_width + KEEP_ROWS),
            ],
            scratch_shapes=[
                pltpu.VMEM((rows + 8, max(tile_lanes, 2 * state_width)), f32),
                pltpu.VMEM((3, rows, LANES), f32),
                pltpu.VMEM((rows, LANES), bf16),
                pltpu.VMEM((rows, LANES), bf16),
                pltpu.VMEM((max(8, blocks + 1), LANES), f32),
                pltpu.VMEM((rows + HALO, depth), bf16),
                pltpu.VMEM((rows, tile_lanes), bf16),
                pltpu.VMEM((rows, tile_lanes), f32),
                pltpu.VMEM((rows, tile_lanes), f32),
                pltpu.VMEM((SLOTS, depth, tile_lanes), bf16),
                pltpu.SemaphoreType.DMA((SLOTS,)),
                pltpu.SemaphoreType.DMA,
            ],
        ),
        out_shape=[
            jax.ShapeDtypeStruct((rows + HALO, depth), bf16),
            jax.ShapeDtypeStruct((tiles, rows, tile_lanes), bf16),
            jax.ShapeDtypeStruct((tiles, rows, tile_lanes), bf16),
            jax.ShapeDtypeStruct((rows, 2 * state_width), bf16),
            jax.ShapeDtypeStruct((rows, LANES), f32),
            jax.ShapeDtypeStruct((LANES, rows), f32),
            jax.ShapeDtypeStruct((rows, LANES), bf16),
            jax.ShapeDtypeStruct((rows, LANES), bf16),
            jax.ShapeDtypeStruct((max(blocks - 1, 1), state_width, channels), bf16),
            jax.ShapeDtypeStruct((state_width + KEEP_ROWS, channels), bf16),
        ],
        compiler_params=pltpu.CompilerParams(
            dimension_semantics=("arbitrary",), vmem_limit_bytes=60 * 2**20
        ),
        cost_estimate=cost(15),
        name="scan",
    )(at, *parts, *halos, gain, wbc, wdt, w_zx, tapx, tapbc, biasx, biasbc, dtb, rate, idc)


def inner_kernel(
    rows,
    heads,
    width,
    x_ref,
    xs_ref,
    bc_ref,
    acol_ref,
    arow_ref,
    ein_ref,
    state_ref,
    skip_ref,
    idc_ref,
    idr_ref,
    y_ref,
    gram,
    mix,
):
    blocks = rows // BLOCK
    state_width = bc_ref.shape[1] // 2

    @pl.when(pl.program_id(0) == 0)
    def _():
        at = lax.broadcasted_iota(jnp.int32, (BLOCK, BLOCK), 0)
        to = lax.broadcasted_iota(jnp.int32, (BLOCK, BLOCK), 1)
        for block in range(blocks):
            r0, r1 = block * BLOCK, (block + 1) * BLOCK
            b_rows = bc_ref[r0:r1, 0:state_width]
            c_rows = bc_ref[r0:r1, state_width:]
            ids = jnp.concatenate([idc_ref[8 + r0 : 8 + r1]] * (BLOCK // LANES), 1)
            same = (at >= to) & (ids == idr_ref[0:1, r0:r1])
            product = lax.dot_general(
                c_rows, b_rows, (((1,), (1,)), ((), ())), preferred_element_type=f32
            )
            gram[block] = jnp.where(same, product, 0.0)

    tile = pl.program_id(0)
    spread = spread_matrix(heads, width, tile)
    acol = pltpu.roll(acol_ref[...], lax.rem(LANES - tile * heads, LANES), 1)
    lane = lax.broadcasted_iota(jnp.int32, (BLOCK, LANES), 1)
    pack = LANES // width
    for block in range(blocks):
        r0, r1 = block * BLOCK, (block + 1) * BLOCK
        if block > 0:
            carried = dot(bc_ref[r0:r1, state_width:], state_ref[block - 1])
            carried = carried * dot(ein_ref[r0:r1], spread)
        for first in range(0, heads, pack):
            cols = slice(first * width, (first + pack) * width)
            xs_now = xs_ref[r0:r1, cols]
            total = None
            for inner in range(pack):
                head = first + inner
                row = arow_ref[head : head + 1, r0:r1]
                for a in range(0, BLOCK, STRIP):
                    gap = acol[r0 + a : r0 + a + STRIP, head : head + 1] - row
                    weight = jnp.exp(jnp.minimum(gap, 0.0)) * gram[block, a : a + STRIP]
                    mix[head % 4, a : a + STRIP] = weight.astype(bf16)
                part = dot(mix[head % 4], xs_now)
                total = part if total is None else jnp.where(lane < inner * width, total, part)
            total = total + skip_ref[:, cols] * x_ref[r0:r1, cols].astype(f32)
            if block > 0:
                total = total + carried[:, cols]
            y_ref[r0:r1, cols] = total.astype(bf16)


def inner_call(x, xs, bc, acol, arow, ein, states, skip, idc, idr, sizes):
    rows, heads, width, tiles, state_width = sizes
    tile_lanes = heads * width
    blocks = rows // BLOCK

    def whole(*shape):
        return pl.BlockSpec(shape, lambda i: (0,) * len(shape))

    def column(lead):
        return pl.BlockSpec((lead, tile_lanes), lambda i: (0, i))

    tiled = pl.BlockSpec((None, rows, tile_lanes), lambda i: (i, 0, 0))
    arow_rows = heads if heads % 8 == 0 else LANES

    return pl.pallas_call(
        functools.partial(inner_kernel, rows, heads, width),
        grid=(tiles,),
        in_specs=[
            tiled,
            tiled,
            whole(rows, 2 * state_width),
            whole(rows, LANES),
            pl.BlockSpec((arow_rows, rows), lambda i: (i, 0)),
            whole(rows, LANES),
            pl.BlockSpec((max(blocks - 1, 1), state_width, tile_lanes), lambda i: (0, 0, i)),
            column(1),
            whole(rows + 8, LANES),
            whole(8, rows),
        ],
        out_specs=tiled,
        out_shape=jax.ShapeDtypeStruct((tiles, rows, tile_lanes), bf16),
        scratch_shapes=[
            pltpu.VMEM((blocks, BLOCK, BLOCK), f32),
            pltpu.VMEM((4, BLOCK, BLOCK), bf16),
        ],
        compiler_params=pltpu.CompilerParams(
            dimension_semantics=("arbitrary",), vmem_limit_bytes=60 * 2**20
        ),
        cost_estimate=cost(11),
        name="inner",
    )(x, xs, bc, acol, arow, ein, states, skip, idc, idr)


def gate_kernel(tiles, normed_ref, wz_ref, gate_ref, held, sems):
    depth, tile_lanes = held.shape[1:]
    place = column_tile(depth, tile_lanes, 0)
    weights = stream(pl.program_id(0), tiles, wz_ref, held, sems, place)
    gate_ref[...] = silu(dot(normed_ref[...], weights[...])).astype(bf16)


def gate_call(normed, w_zx, sizes):
    rows, heads, width, tiles, _ = sizes
    depth = normed.shape[1]
    tile_lanes = heads * width
    return pl.pallas_call(
        functools.partial(gate_kernel, tiles),
        grid=(tiles,),
        in_specs=[
            pl.BlockSpec((rows, depth), lambda i: (0, 0)),
            pl.BlockSpec(memory_space=pltpu.HBM),
        ],
        scratch_shapes=[
            pltpu.VMEM((SLOTS, depth, tile_lanes), bf16),
            pltpu.SemaphoreType.DMA((SLOTS,)),
        ],
        out_specs=pl.BlockSpec((None, rows, tile_lanes), lambda i: (i, 0, 0)),
        out_shape=jax.ShapeDtypeStruct((tiles, rows, tile_lanes), bf16),
        compiler_params=pltpu.CompilerParams(
            dimension_semantics=("arbitrary",), vmem_limit_bytes=60 * 2**20
        ),
        cost_estimate=cost(8),
        name="gate",
    )(normed, w_zx)


def out_kernel(
    heads,
    width,
    at_ref,
    y_ref,
    gate_ref,
    bc_ref,
    eall_ref,
    stay_ref,
    got_ref,
    gain_ref,
    w_ref,
    p_ref,
    sq_ref,
    lhs,
    coming,
    held,
    sems,
):
    state_width = bc_ref.shape[1] // 2
    half = stay_ref.shape[1]
    tiles, _, tile_lanes = y_ref.shape
    piece = pl.program_id(0)
    channels, lanes = held.shape[1:]

    def prepare():
        swapped = at_ref[1] != 0
        coming[:, :half] = jnp.where(swapped, got_ref[...], stay_ref[...])
        coming[:, half:] = jnp.where(swapped, stay_ref[...], got_ref[...])
        squares = None
        for tile in range(tiles):
            cols = slice(tile * tile_lanes, (tile + 1) * tile_lanes)
            carried = dot(bc_ref[:, state_width:], coming[:, cols])
            carried = carried * dot(eall_ref[...], spread_matrix(heads, width, tile))
            gated = (y_ref[tile].astype(f32) + carried) * gate_ref[tile].astype(f32)
            part = jnp.sum(gated * gated, axis=1, keepdims=True)
            squares = part if squares is None else squares + part
            lhs[:, cols] = (gated * gain_ref[:, cols]).astype(bf16)
        sq_ref[...] = jnp.broadcast_to(squares, sq_ref.shape)

    weights = stream(
        piece, w_ref.shape[1] // lanes, w_ref, held, sems, column_tile(channels, lanes, 0), prepare
    )
    p_ref[...] = dot(lhs[...], weights[...]).astype(bf16)


def out_call(at, y, gate, bc, eall, stay, got, gain, w_out, count, sizes):
    rows, heads, width, tiles, state_width = sizes
    channels, depth = w_out.shape
    tile_lanes = heads * width

    def taken(lanes):
        return pl.BlockSpec((count, lanes), lambda i, at: (at[0], 0))

    def whole(*shape):
        return pl.BlockSpec(shape, lambda i, at: (0,) * len(shape))

    piece = 512 if depth % 512 == 0 else depth
    tiled = pl.BlockSpec((tiles, count, tile_lanes), lambda i, at: (0, at[0], 0))
    return pl.pallas_call(
        functools.partial(out_kernel, heads, width),
        grid_spec=pltpu.PrefetchScalarGridSpec(
            num_scalar_prefetch=1,
            grid=(depth // piece,),
            in_specs=[
                tiled,
                tiled,
                taken(2 * state_width),
                taken(LANES),
                whole(state_width, channels // 2),
                whole(state_width, channels // 2),
                whole(1, channels),
                pl.BlockSpec(memory_space=pltpu.HBM),
            ],
            out_specs=[
                pl.BlockSpec((count, piece), lambda i, at: (0, i)),
                whole(count, LANES),
            ],
            scratch_shapes=[
                pltpu.VMEM((count, channels), bf16),
                pltpu.VMEM((state_width, channels), bf16),
                pltpu.VMEM((SLOTS, channels, piece), bf16),
                pltpu.SemaphoreType.DMA((SLOTS,)),
            ],
        ),
        out_shape=[
            jax.ShapeDtypeStruct((count, depth), bf16),
            jax.ShapeDtypeStruct((count, LANES), f32),
        ],
        compiler_params=pltpu.CompilerParams(
            dimension_semantics=("arbitrary",), vmem_limit_bytes=60 * 2**20
        ),
        cost_estimate=cost(6),
        name="outp",
    )(at, y, gate, bc, eall, stay, got, gain, w_out)


class Route:
    def __init__(self, sizes):
        self.pipes, self.seqs, self.tps = sizes

    def spot(self, pipe, seq, tp):
        return (pipe * self.seqs + seq) * self.tps + tp

    def move(self, block, pairs):
        return lax.ppermute(
            block, AXES, [(self.spot(*source), self.spot(*target)) for source, target in pairs]
        )

    def every(self):
        return [(s, t) for s in range(self.seqs) for t in range(self.tps)]


def gather_rows(route, own, source_pipe, pipe, tail_after=None, ids_row=None):
    tps, seqs = route.tps, route.seqs
    parts = [own]
    if source_pipe != pipe:
        parts = [route.move(own, [((source_pipe, s, t), (pipe, s, t)) for s, t in route.every()])]
    for distance in range(1, tps):
        parts.append(
            route.move(
                own,
                [
                    ((source_pipe, s, (t + distance) % tps), (pipe, s, t))
                    for s, t in route.every()
                ],
            )
        )
    tail = own[own.shape[0] - HALO :]
    if ids_row is not None:
        tail = jnp.concatenate([tail, ids_row], 0)
    pipes = [(source_pipe, pipe)] if ids_row is None else [(p, p) for p in range(route.pipes)]
    halos = [
        route.move(
            tail,
            [((a, s, tps - 1), (b, s + 1, t)) for a, b in pipes for s in range(seqs - 1)],
        )
        for t in range(tps)
    ]
    return parts, halos


def exchange_states(route, sent, state_width, pipe, under_swap, under_scan, scan_inputs):
    seqs = route.seqs
    outer, side = seqs // 2, lax.axis_index("seq") % 2
    half = sent.shape[1] // 2
    is_first = side == 0

    def swap(block):
        return route.move(
            block, [((pipe, s, t), (pipe, s + 1 - 2 * (s % 2), t)) for s, t in route.every()]
        )

    def parted(block):
        block = block.astype(f32)
        keep = block[state_width : state_width + 1] + block[state_width + 1 : state_width + 2]
        return block[:state_width], keep

    def joined(state, keep):
        high = keep.astype(bf16)
        low = (keep - high.astype(f32)).astype(bf16)
        rest = jnp.zeros((KEEP_ROWS - 2, half), bf16)
        return jnp.concatenate([state.astype(bf16), high, low, rest], 0)

    low, high = sent[:, :half], sent[:, half:]
    mine = jnp.where(is_first, low, high)
    theirs = swap(jnp.where(is_first, high, low))
    theirs, gate = lax.optimization_barrier((theirs, under_swap()))
    early, keep_early = parted(jnp.where(is_first, mine, theirs))
    late, keep_late = parted(jnp.where(is_first, theirs, mine))
    pair = joined(keep_late * early + late, keep_early * keep_late)
    pair, scan_inputs = lax.optimization_barrier((pair, scan_inputs))
    arrivals = []
    for distance in range(1, outer):
        pairs = [
            ((pipe, s - 2 * distance, t), (pipe, s, t))
            for s, t in route.every()
            if s - 2 * distance >= 0
        ]
        arrivals.append(route.move(pair, pairs))
    arrivals, mixed = lax.optimization_barrier((arrivals, under_scan(*scan_inputs)))
    total, weight = parted(arrivals[0])
    for came in arrivals[1:]:
        came, keep_came = parted(came)
        total = total + weight * came
        weight = weight * keep_came
    after_early = keep_early * total + early
    stay = jnp.where(is_first, total, after_early).astype(bf16)
    got = swap(jnp.where(is_first, after_early, total).astype(bf16))
    return stay, got, gate, mixed


def local(
    hidden_in,
    doc_ids,
    norm_gain,
    in_zx,
    in_bc,
    in_dt,
    conv_x,
    conv_bc,
    bias_x,
    bias_bc,
    dt_bias,
    a_log,
    d_skip,
    gated_gain,
    out_w,
):
    route = Route(tuple(lax.axis_size(a) for a in AXES))
    section = lax.axis_index("pipe")
    tp = lax.axis_index("tp")
    micro_count = hidden_in.shape[0]
    channels = gated_gain.shape[1]
    local_heads = dt_bias.shape[1]
    width = channels // local_heads
    depth = in_zx.shape[1]
    rows = doc_ids.shape[1]
    own_rows = hidden_in.shape[1]
    state_width = in_bc.shape[2] // 2
    heads = 8 if local_heads % 8 == 0 else local_heads
    tiles = local_heads // heads
    sizes = (rows, heads, width, tiles, state_width)
    full_width = channels * route.tps

    def lanes(a):
        return jnp.pad(a, ((0, 0), (0, LANES - local_heads)))

    w_zx = in_zx[0].reshape(depth, 2 * channels)
    wdt = jnp.pad(in_dt[0].T, ((0, LANES - local_heads), (0, 0)))
    dtb = lanes(dt_bias)
    rate = lanes(-jnp.exp(a_log))
    skip = jnp.repeat(d_skip, width, axis=1)
    every = route.every()
    outputs = []
    for micro in range(micro_count):
        ids = doc_ids[micro].astype(f32)
        ids_row = jnp.broadcast_to(
            jnp.pad(ids[rows - 8 :], (0, depth - 8)).astype(bf16)[None, :], (HALO, depth)
        )
        current = hidden_in[micro]
        source = 0
        result = jnp.zeros_like(current)
        for pipe in range(route.pipes):
            if source == pipe:
                parts, halos = gather_rows(route, current, source, pipe, None, ids_row)
                before = sum(h[HALO, :8].astype(f32) for h in halos)
                before = jnp.where(lax.axis_index("seq") == 0, -1.0, before)
                idc = jnp.broadcast_to(
                    jnp.concatenate([before, ids])[:, None], (rows + 8, LANES)
                )
                idr = jnp.broadcast_to(ids[None, :], (8, rows))
            else:
                parts, halos = gather_rows(route, current, source, pipe)
            residual = parts[0]
            at = ((tp + jnp.arange(route.tps, dtype=jnp.int32)) % route.tps) * own_rows
            normed, x, xs, bc, acol, arow, ein, eall, states, sent = scan_call(
                at,
                parts,
                halos,
                norm_gain,
                in_bc[0],
                wdt,
                w_zx,
                conv_x[0],
                conv_bc[0],
                bias_x,
                bias_bc,
                dtb,
                rate,
                idc,
                sizes,
            )
            stay, got, gate, y = exchange_states(
                route,
                sent,
                state_width,
                pipe,
                lambda: gate_call(normed, w_zx, sizes),
                lambda *a: inner_call(*a, bc, acol, arow, ein, states, skip, idc, idr, sizes),
                (x, xs),
            )
            swapped = lax.axis_index("seq") % 2
            total = None
            squares = None
            for distance in range(1, route.tps):
                at = jnp.stack([(tp + distance) % route.tps, swapped]).astype(jnp.int32)
                part, sq = out_call(
                    at, y, gate, bc, eall, stay, got, gated_gain, out_w[0], own_rows, sizes
                )
                pairs = [
                    ((pipe, s, t), (pipe, s, (t + distance) % route.tps)) for s, t in every
                ]
                part = route.move(part, pairs).astype(f32)
                sq = route.move(sq, pairs)
                total = part if total is None else total + part
                squares = sq if squares is None else squares + sq
            part, sq = out_call(
                jnp.stack([tp, swapped]).astype(jnp.int32),
                y, gate, bc, eall, stay, got, gated_gain, out_w[0], own_rows, sizes
            )
            total = part.astype(f32) if total is None else total + part.astype(f32)
            squares = sq if squares is None else squares + sq
            scale = lax.rsqrt(squares[:, 0:1] / full_width + epsilon)
            current = (residual.astype(f32) + scale * total).astype(bf16)
            source = pipe
            result = jnp.where(section == pipe, current, result)
        outputs.append(result)
    return jnp.stack(outputs)[None]


def solution(mesh):
    placed = (
        P(None, ("seq", "tp"), None),
        P(None, "seq"),
        P("pipe", None),
        P("pipe", None, None, "tp"),
        P("pipe", None, None),
        P("pipe", None, "tp"),
        P("pipe", None, "tp"),
        P("pipe", None, None),
        P("pipe", "tp"),
        P("pipe", None),
        P("pipe", "tp"),
        P("pipe", "tp"),
        P("pipe", "tp"),
        P("pipe", "tp"),
        P("pipe", "tp", None),
    )
    return jax.shard_map(
        local,
        mesh=mesh,
        in_specs=placed,
        out_specs=P("pipe", None, ("seq", "tp"), None),
        check_vma=False,
    )
```

```python
import functools

import jax
import jax.numpy as jnp
from jax import lax
from jax.experimental import pallas as pl
from jax.experimental.pallas import tpu as pltpu
from jax.sharding import PartitionSpec as P

AXES = ("pipe", "seq", "tp")
BLOCK = 256
HALO = 16
KEEP_ROWS = 16
SLOTS = 3
STRIP = 64
LANES = 128
epsilon = 1e-05
highest = lax.Precision.HIGHEST
f32 = jnp.float32
bf16 = jnp.bfloat16


def dot(a, b):
    return jnp.dot(a, b, preferred_element_type=f32)


def cost(micros):
    return pl.CostEstimate(flops=int(micros * 2.5e8), bytes_accessed=0, transcendentals=0)


def silu(v):
    half = 0.5 * v
    return half + half * jnp.tanh(half)


def softplus(v):
    return jnp.maximum(v, 0.0) + jnp.log1p(jnp.exp(-jnp.abs(v)))


def spread_matrix(heads, width, tile):
    rows = lax.broadcasted_iota(jnp.int32, (LANES, heads * width), 0) - tile * heads
    cols = lax.broadcasted_iota(jnp.int32, (LANES, heads * width), 1)
    inside = (cols >= rows * width) & (cols < (rows + 1) * width)
    return jnp.where(inside, 1.0, 0.0).astype(bf16)


def stream(step_at, count, source, held, sems, place, meanwhile=None):
    slots = held.shape[0]

    def copy(tile):
        slot = lax.rem(tile, slots)
        return pltpu.make_async_copy(source.at[place(tile)], held.at[slot], sems.at[slot])

    @pl.when(step_at == 0)
    def _():
        for tile in range(min(slots - 1, count)):
            copy(tile).start()
        if meanwhile is not None:
            meanwhile()

    if count >= slots:

        @pl.when(step_at + slots - 1 < count)
        def _():
            copy(step_at + slots - 1).start()

    copy(step_at).wait()
    return held.at[lax.rem(step_at, slots)]


def column_tile(depth, lanes, first):
    return lambda tile: (
        pl.ds(0, depth),
        pl.ds(pl.multiple_of(first + tile * lanes, LANES), lanes),
    )


def conv_rows(raw_ref, keep_ref, taps, bias, start, stop, col):
    width = LANES
    out = bias + taps[3:4] * raw_ref[start + 8 : stop + 8, col : col + width]
    for tap in range(3):
        shifted_rows = raw_ref[start + 5 + tap : stop + 5 + tap, col : col + width]
        out = out + keep_ref[tap, start:stop] * (taps[tap : tap + 1] * shifted_rows)
    return silu(out)


def scan_kernel(rows, heads, width, shares, at_ref, *refs):
    part_refs, halo_refs = refs[:shares], refs[shares : 2 * shares]
    (
        gain_ref,
        wbc_ref,
        wdt_ref,
        wx_ref,
        tapx_ref,
        tapbc_ref,
        biasx_ref,
        biasbc_ref,
        dtb_ref,
        rate_ref,
        idc_ref,
        normed_ref,
        x_ref,
        bc_ref,
        acol_ref,
        arow_ref,
        srow_ref,
        ein_ref,
        eall_ref,
        state_ref,
        sent_ref,
        raw,
        keep,
        wend,
        kept,
        lhs,
        weighted,
        wend_lanes,
        held,
        sems,
        out_sem,
    ) = refs[2 * shares :]
    step_at = pl.program_id(0)
    blocks = rows // BLOCK
    state_width = bc_ref.shape[1] // 2
    tile_lanes = heads * width
    unit = 256 if tile_lanes % 256 == 0 else LANES
    units = tile_lanes // unit

    saved = pltpu.make_async_copy(lhs, normed_ref, out_sem)

    def first():
        gain = gain_ref[...]

        def normalize(part):
            scale = lax.rsqrt(jnp.mean(part * part, axis=1, keepdims=True) + epsilon)
            return (part * scale * gain).astype(bf16)

        for share in range(shares):
            for begin in range(0, rows // shares, HALO):
                place = pl.multiple_of(at_ref[share] + begin, HALO)
                part = part_refs[share][begin : begin + HALO].astype(f32)
                lhs[pl.ds(place, HALO)] = normalize(part)
        halo = halo_refs[0][...].astype(f32)
        for other in halo_refs[1:]:
            halo = halo + other[...].astype(f32)
        lhs[rows:] = normalize(halo)
        saved.start()
        small = dot(lhs[...], wbc_ref[...])
        dt_raw = lax.dot_general(
            lhs[0:rows], wdt_ref[...], (((1,), (1,)), ((), ())), preferred_element_type=f32
        )
        for tap in range(3):
            keep[tap] = (idc_ref[5 + tap : 5 + tap + rows] == idc_ref[8 : 8 + rows]).astype(f32)
        raw[0:8, 0 : 2 * state_width] = small[rows + HALO - 8 :]
        raw[8 : 8 + rows, 0 : 2 * state_width] = small[:rows]
        for col in range(0, 2 * state_width, LANES):
            strip_cols = slice(col, col + LANES)
            for a in range(0, rows, STRIP):
                bc_ref[a : a + STRIP, strip_cols] = conv_rows(
                    raw,
                    keep,
                    tapbc_ref[:, strip_cols],
                    biasbc_ref[:, strip_cols],
                    a,
                    a + STRIP,
                    col,
                ).astype(bf16)
        step = softplus(dt_raw + dtb_ref[...])
        log_step = step * rate_ref[...]
        at = lax.broadcasted_iota(jnp.int32, (BLOCK, BLOCK), 0)
        to = lax.broadcasted_iota(jnp.int32, (BLOCK, BLOCK), 1)
        lower = (at >= to).astype(f32)
        first_prev = idc_ref[7:8]
        before = jnp.zeros((1, LANES), f32)
        kept[...] = jnp.zeros_like(kept)
        for block in range(blocks):
            r0, r1 = block * BLOCK, (block + 1) * BLOCK
            ids = idc_ref[8 + r0 : 8 + r1]
            prev = idc_ref[7 + r0 : 8 + r0]
            last = idc_ref[7 + r1 : 8 + r1]
            part_step = step[r0:r1]
            total = jnp.dot(lower, log_step[r0:r1], precision=highest, preferred_element_type=f32)
            end = total[BLOCK - 1 : BLOCK]
            acol_ref[r0:r1] = total
            arow_ref[:, r0:r1] = total.T
            srow_ref[:, r0:r1] = part_step.T
            ein_ref[r0:r1] = (jnp.exp(total) * (ids == prev).astype(f32)).astype(bf16)
            eall_ref[r0:r1] = (jnp.exp(total + before) * (ids == first_prev).astype(f32)).astype(
                bf16
            )
            wend[r0:r1] = (jnp.exp(end - total) * (ids == last).astype(f32) * part_step).astype(
                bf16
            )
            kept[block : block + 1] = jnp.exp(end) * (last == prev).astype(f32)
            before = before + end
        kept[blocks : blocks + 1] = jnp.exp(before) * (
            idc_ref[7 + rows : 8 + rows] == first_prev
        ).astype(f32)

    depth = wx_ref.shape[0]
    tiles = wx_ref.shape[1] // (2 * tile_lanes)
    place = column_tile(depth, tile_lanes, tiles * tile_lanes)
    weights = stream(step_at, tiles, wx_ref, held, sems, place, first)
    spread = spread_matrix(heads, width, step_at)
    kept_now = kept[...]
    high = kept_now.astype(bf16)
    low = (kept_now - high.astype(f32)).astype(bf16)
    keep_lanes = dot(high, spread) + dot(low, spread)
    wend_lanes[...] = dot(wend[...], spread)
    for u in range(units):
        cols = slice(u * unit, (u + 1) * unit)
        fresh = dot(lhs[...], weights[:, cols])
        raw[0:8, cols] = fresh[rows + HALO - 8 :]
        raw[8 : 8 + rows, cols] = fresh[:rows]
    at = lax.broadcasted_iota(jnp.int32, (KEEP_ROWS, unit), 0)
    for u in range(units):
        cols = slice(u * unit, (u + 1) * unit)
        running = None
        for block in range(blocks):
            r0, r1 = block * BLOCK, (block + 1) * BLOCK
            for col in range(u * unit, (u + 1) * unit, LANES):
                strip_cols = slice(col, col + LANES)
                taps = tapx_ref[:, strip_cols]
                bias = biasx_ref[:, strip_cols]
                for a in range(r0, r1, STRIP):
                    b = a + STRIP
                    x_now = conv_rows(raw, keep, taps, bias, a, b, col)
                    x_ref[a:b, strip_cols] = x_now.astype(bf16)
                    weighted[a:b, strip_cols] = (x_now * wend_lanes[a:b, strip_cols]).astype(bf16)
            local = lax.dot_general(
                bc_ref[r0:r1, 0:state_width],
                weighted[r0:r1, cols],
                (((0,), (0,)), ((), ())),
                preferred_element_type=f32,
            )
            if running is not None:
                local = local + keep_lanes[block : block + 1, cols] * running
            running = local
            if block < blocks - 1:
                state_ref[block, :, cols] = running.astype(bf16)
        sent_ref[0:state_width, cols] = running.astype(bf16)
        shard_row = keep_lanes[blocks : blocks + 1, cols]
        shard_high = shard_row.astype(bf16).astype(f32)
        both = jnp.where(
            at == 0, shard_high, jnp.where(at == 1, shard_row - shard_high, 0.0)
        )
        sent_ref[state_width:, cols] = both.astype(bf16)

    @pl.when(step_at == pl.num_programs(0) - 1)
    def _():
        saved.wait()


def scan_call(at, parts, halos, gain, wbc, wdt, w_zx, tapx, tapbc, biasx, biasbc, dtb, rate, idc, sizes):
    rows, heads, width, tiles, state_width = sizes
    shares, depth = len(parts), w_zx.shape[0]
    tile_lanes = heads * width
    channels = tiles * tile_lanes
    blocks = rows // BLOCK

    def whole(*shape):
        return pl.BlockSpec(shape, lambda i, at: (0,) * len(shape))

    def column(lead):
        return pl.BlockSpec((lead, tile_lanes), lambda i, at: (0, i))

    return pl.pallas_call(
        functools.partial(scan_kernel, rows, heads, width, shares),
        grid_spec=pltpu.PrefetchScalarGridSpec(
            num_scalar_prefetch=1,
            grid=(tiles,),
            in_specs=[whole(rows // shares, depth)] * shares
            + [whole(HALO, depth)] * shares
            + [
                whole(1, depth),
                whole(depth, 2 * state_width),
                whole(LANES, depth),
                pl.BlockSpec(memory_space=pltpu.HBM),
                column(4),
                whole(4, 2 * state_width),
                column(1),
                whole(1, 2 * state_width),
                whole(1, LANES),
                whole(1, LANES),
                whole(rows + 8, LANES),
            ],
            out_specs=[
                pl.BlockSpec(memory_space=pltpu.HBM),
                pl.BlockSpec((None, rows, tile_lanes), lambda i, at: (i, 0, 0)),
                whole(rows, 2 * state_width),
                whole(rows, LANES),
                whole(LANES, rows),
                whole(LANES, rows),
                whole(rows, LANES),
                whole(rows, LANES),
                pl.BlockSpec(
                    (max(blocks - 1, 1), state_width, tile_lanes), lambda i, at: (0, 0, i)
                ),
                column(state_width + KEEP_ROWS),
            ],
            scratch_shapes=[
                pltpu.VMEM((rows + 8, max(tile_lanes, 2 * state_width)), f32),
                pltpu.VMEM((3, rows, LANES), f32),
                pltpu.VMEM((rows, LANES), bf16),
                pltpu.VMEM((max(8, blocks + 1), LANES), f32),
                pltpu.VMEM((rows + HALO, depth), bf16),
                pltpu.VMEM((rows, tile_lanes), bf16),
                pltpu.VMEM((rows, tile_lanes), f32),
                pltpu.VMEM((SLOTS, depth, tile_lanes), bf16),
                pltpu.SemaphoreType.DMA((SLOTS,)),
                pltpu.SemaphoreType.DMA,
            ],
        ),
        out_shape=[
            jax.ShapeDtypeStruct((rows + HALO, depth), bf16),
            jax.ShapeDtypeStruct((tiles, rows, tile_lanes), bf16),
            jax.ShapeDtypeStruct((rows, 2 * state_width), bf16),
            jax.ShapeDtypeStruct((rows, LANES), f32),
            jax.ShapeDtypeStruct((LANES, rows), f32),
            jax.ShapeDtypeStruct((LANES, rows), f32),
            jax.ShapeDtypeStruct((rows, LANES), bf16),
            jax.ShapeDtypeStruct((rows, LANES), bf16),
            jax.ShapeDtypeStruct((max(blocks - 1, 1), state_width, channels), bf16),
            jax.ShapeDtypeStruct((state_width + KEEP_ROWS, channels), bf16),
        ],
        compiler_params=pltpu.CompilerParams(
            dimension_semantics=("arbitrary",), vmem_limit_bytes=60 * 2**20
        ),
        cost_estimate=cost(15),
        name="scan",
    )(at, *parts, *halos, gain, wbc, wdt, w_zx, tapx, tapbc, biasx, biasbc, dtb, rate, idc)


def inner_kernel(
    rows,
    heads,
    width,
    x_ref,
    bc_ref,
    acol_ref,
    arow_ref,
    srow_ref,
    ein_ref,
    state_ref,
    skip_ref,
    idc_ref,
    idr_ref,
    y_ref,
    gram,
    mix,
):
    blocks = rows // BLOCK
    state_width = bc_ref.shape[1] // 2

    @pl.when(pl.program_id(0) == 0)
    def _():
        at = lax.broadcasted_iota(jnp.int32, (BLOCK, BLOCK), 0)
        to = lax.broadcasted_iota(jnp.int32, (BLOCK, BLOCK), 1)
        for block in range(blocks):
            r0, r1 = block * BLOCK, (block + 1) * BLOCK
            b_rows = bc_ref[r0:r1, 0:state_width]
            c_rows = bc_ref[r0:r1, state_width:]
            ids = jnp.concatenate([idc_ref[8 + r0 : 8 + r1]] * (BLOCK // LANES), 1)
            same = (at >= to) & (ids == idr_ref[0:1, r0:r1])
            product = lax.dot_general(
                c_rows, b_rows, (((1,), (1,)), ((), ())), preferred_element_type=f32
            )
            gram[block] = jnp.where(same, product, 0.0)

    tile = pl.program_id(0)
    spread = spread_matrix(heads, width, tile)
    acol = pltpu.roll(acol_ref[...], lax.rem(LANES - tile * heads, LANES), 1)
    lane = lax.broadcasted_iota(jnp.int32, (BLOCK, LANES), 1)
    pack = LANES // width
    for block in range(blocks):
        r0, r1 = block * BLOCK, (block + 1) * BLOCK
        if block > 0:
            carried = dot(bc_ref[r0:r1, state_width:], state_ref[block - 1])
            carried = carried * dot(ein_ref[r0:r1], spread)
        for first in range(0, heads, pack):
            cols = slice(first * width, (first + pack) * width)
            x_now = x_ref[r0:r1, cols]
            total = None
            for inner in range(pack):
                head = first + inner
                row = arow_ref[head : head + 1, r0:r1]
                step = srow_ref[head : head + 1, r0:r1]
                for a in range(0, BLOCK, STRIP):
                    gap = acol[r0 + a : r0 + a + STRIP, head : head + 1] - row
                    weight = jnp.exp(jnp.minimum(gap, 0.0)) * gram[block, a : a + STRIP]
                    mix[head % 4, a : a + STRIP] = (weight * step).astype(bf16)
                part = dot(mix[head % 4], x_now)
                total = part if total is None else jnp.where(lane < inner * width, total, part)
            total = total + skip_ref[:, cols] * x_now.astype(f32)
            if block > 0:
                total = total + carried[:, cols]
            y_ref[r0:r1, cols] = total.astype(bf16)


def inner_call(x, bc, acol, arow, srow, ein, states, skip, idc, idr, sizes):
    rows, heads, width, tiles, state_width = sizes
    tile_lanes = heads * width
    blocks = rows // BLOCK

    def whole(*shape):
        return pl.BlockSpec(shape, lambda i: (0,) * len(shape))

    def column(lead):
        return pl.BlockSpec((lead, tile_lanes), lambda i: (0, i))

    tiled = pl.BlockSpec((None, rows, tile_lanes), lambda i: (i, 0, 0))
    arow_rows = heads if heads % 8 == 0 else LANES

    return pl.pallas_call(
        functools.partial(inner_kernel, rows, heads, width),
        grid=(tiles,),
        in_specs=[
            tiled,
            whole(rows, 2 * state_width),
            whole(rows, LANES),
            pl.BlockSpec((arow_rows, rows), lambda i: (i, 0)),
            pl.BlockSpec((arow_rows, rows), lambda i: (i, 0)),
            whole(rows, LANES),
            pl.BlockSpec((max(blocks - 1, 1), state_width, tile_lanes), lambda i: (0, 0, i)),
            column(1),
            whole(rows + 8, LANES),
            whole(8, rows),
        ],
        out_specs=tiled,
        out_shape=jax.ShapeDtypeStruct((tiles, rows, tile_lanes), bf16),
        scratch_shapes=[
            pltpu.VMEM((blocks, BLOCK, BLOCK), f32),
            pltpu.VMEM((4, BLOCK, BLOCK), bf16),
        ],
        compiler_params=pltpu.CompilerParams(
            dimension_semantics=("arbitrary",), vmem_limit_bytes=60 * 2**20
        ),
        cost_estimate=cost(11),
        name="inner",
    )(x, bc, acol, arow, srow, ein, states, skip, idc, idr)


def gate_kernel(tiles, normed_ref, wz_ref, gate_ref, held, sems):
    depth, tile_lanes = held.shape[1:]
    place = column_tile(depth, tile_lanes, 0)
    weights = stream(pl.program_id(0), tiles, wz_ref, held, sems, place)
    gate_ref[...] = silu(dot(normed_ref[...], weights[...])).astype(bf16)


def gate_call(normed, w_zx, sizes):
    rows, heads, width, tiles, _ = sizes
    depth = normed.shape[1]
    tile_lanes = heads * width
    return pl.pallas_call(
        functools.partial(gate_kernel, tiles),
        grid=(tiles,),
        in_specs=[
            pl.BlockSpec((rows, depth), lambda i: (0, 0)),
            pl.BlockSpec(memory_space=pltpu.HBM),
        ],
        scratch_shapes=[
            pltpu.VMEM((SLOTS, depth, tile_lanes), bf16),
            pltpu.SemaphoreType.DMA((SLOTS,)),
        ],
        out_specs=pl.BlockSpec((None, rows, tile_lanes), lambda i: (i, 0, 0)),
        out_shape=jax.ShapeDtypeStruct((tiles, rows, tile_lanes), bf16),
        compiler_params=pltpu.CompilerParams(
            dimension_semantics=("arbitrary",), vmem_limit_bytes=60 * 2**20
        ),
        cost_estimate=cost(8),
        name="gate",
    )(normed, w_zx)


def out_kernel(
    heads,
    width,
    at_ref,
    y_ref,
    gate_ref,
    bc_ref,
    eall_ref,
    stay_ref,
    got_ref,
    gain_ref,
    w_ref,
    p_ref,
    sq_ref,
    lhs,
    coming,
    held,
    sems,
):
    state_width = bc_ref.shape[1] // 2
    half = stay_ref.shape[1]
    tiles, _, tile_lanes = y_ref.shape
    piece = pl.program_id(0)
    channels, lanes = held.shape[1:]

    def prepare():
        swapped = at_ref[1] != 0
        coming[:, :half] = jnp.where(swapped, got_ref[...], stay_ref[...])
        coming[:, half:] = jnp.where(swapped, stay_ref[...], got_ref[...])
        squares = None
        for tile in range(tiles):
            cols = slice(tile * tile_lanes, (tile + 1) * tile_lanes)
            carried = dot(bc_ref[:, state_width:], coming[:, cols])
            carried = carried * dot(eall_ref[...], spread_matrix(heads, width, tile))
            gated = (y_ref[tile].astype(f32) + carried) * gate_ref[tile].astype(f32)
            part = jnp.sum(gated * gated, axis=1, keepdims=True)
            squares = part if squares is None else squares + part
            lhs[:, cols] = (gated * gain_ref[:, cols]).astype(bf16)
        sq_ref[...] = jnp.broadcast_to(squares, sq_ref.shape)

    weights = stream(
        piece, w_ref.shape[1] // lanes, w_ref, held, sems, column_tile(channels, lanes, 0), prepare
    )
    p_ref[...] = dot(lhs[...], weights[...]).astype(bf16)


def out_call(at, y, gate, bc, eall, stay, got, gain, w_out, count, sizes):
    rows, heads, width, tiles, state_width = sizes
    channels, depth = w_out.shape
    tile_lanes = heads * width

    def taken(lanes):
        return pl.BlockSpec((count, lanes), lambda i, at: (at[0], 0))

    def whole(*shape):
        return pl.BlockSpec(shape, lambda i, at: (0,) * len(shape))

    piece = 512 if depth % 512 == 0 else depth
    tiled = pl.BlockSpec((tiles, count, tile_lanes), lambda i, at: (0, at[0], 0))
    return pl.pallas_call(
        functools.partial(out_kernel, heads, width),
        grid_spec=pltpu.PrefetchScalarGridSpec(
            num_scalar_prefetch=1,
            grid=(depth // piece,),
            in_specs=[
                tiled,
                tiled,
                taken(2 * state_width),
                taken(LANES),
                whole(state_width, channels // 2),
                whole(state_width, channels // 2),
                whole(1, channels),
                pl.BlockSpec(memory_space=pltpu.HBM),
            ],
            out_specs=[
                pl.BlockSpec((count, piece), lambda i, at: (0, i)),
                whole(count, LANES),
            ],
            scratch_shapes=[
                pltpu.VMEM((count, channels), bf16),
                pltpu.VMEM((state_width, channels), bf16),
                pltpu.VMEM((SLOTS, channels, piece), bf16),
                pltpu.SemaphoreType.DMA((SLOTS,)),
            ],
        ),
        out_shape=[
            jax.ShapeDtypeStruct((count, depth), bf16),
            jax.ShapeDtypeStruct((count, LANES), f32),
        ],
        compiler_params=pltpu.CompilerParams(
            dimension_semantics=("arbitrary",), vmem_limit_bytes=60 * 2**20
        ),
        cost_estimate=cost(6),
        name="outp",
    )(at, y, gate, bc, eall, stay, got, gain, w_out)


class Route:
    def __init__(self, sizes):
        self.pipes, self.seqs, self.tps = sizes

    def spot(self, pipe, seq, tp):
        return (pipe * self.seqs + seq) * self.tps + tp

    def move(self, block, pairs):
        return lax.ppermute(
            block, AXES, [(self.spot(*source), self.spot(*target)) for source, target in pairs]
        )

    def every(self):
        return [(s, t) for s in range(self.seqs) for t in range(self.tps)]


def gather_rows(route, own, source_pipe, pipe, tail_after=None, ids_row=None):
    tps, seqs = route.tps, route.seqs
    parts = [own]
    if source_pipe != pipe:
        parts = [route.move(own, [((source_pipe, s, t), (pipe, s, t)) for s, t in route.every()])]
    for distance in range(1, tps):
        parts.append(
            route.move(
                own,
                [
                    ((source_pipe, s, (t + distance) % tps), (pipe, s, t))
                    for s, t in route.every()
                ],
            )
        )
    tail = own[own.shape[0] - HALO :]
    if ids_row is not None:
        tail = jnp.concatenate([tail, ids_row], 0)
    pipes = [(source_pipe, pipe)] if ids_row is None else [(p, p) for p in range(route.pipes)]
    halos = [
        route.move(
            tail,
            [((a, s, tps - 1), (b, s + 1, t)) for a, b in pipes for s in range(seqs - 1)],
        )
        for t in range(tps)
    ]
    return parts, halos


def exchange_states(route, sent, state_width, pipe, under_swap, under_scan, scan_inputs):
    seqs = route.seqs
    outer, side = seqs // 2, lax.axis_index("seq") % 2
    half = sent.shape[1] // 2
    is_first = side == 0

    def swap(block):
        return route.move(
            block, [((pipe, s, t), (pipe, s + 1 - 2 * (s % 2), t)) for s, t in route.every()]
        )

    def parted(block):
        block = block.astype(f32)
        keep = block[state_width : state_width + 1] + block[state_width + 1 : state_width + 2]
        return block[:state_width], keep

    def joined(state, keep):
        high = keep.astype(bf16)
        low = (keep - high.astype(f32)).astype(bf16)
        rest = jnp.zeros((KEEP_ROWS - 2, half), bf16)
        return jnp.concatenate([state.astype(bf16), high, low, rest], 0)

    low, high = sent[:, :half], sent[:, half:]
    mine = jnp.where(is_first, low, high)
    theirs = swap(jnp.where(is_first, high, low))
    theirs, gate = lax.optimization_barrier((theirs, under_swap()))
    early, keep_early = parted(jnp.where(is_first, mine, theirs))
    late, keep_late = parted(jnp.where(is_first, theirs, mine))
    pair = joined(keep_late * early + late, keep_early * keep_late)
    pair, scan_inputs = lax.optimization_barrier((pair, scan_inputs))
    arrivals = []
    for distance in range(1, outer):
        pairs = [
            ((pipe, s - 2 * distance, t), (pipe, s, t))
            for s, t in route.every()
            if s - 2 * distance >= 0
        ]
        arrivals.append(route.move(pair, pairs))
    arrivals, mixed = lax.optimization_barrier((arrivals, under_scan(*scan_inputs)))
    total, weight = parted(arrivals[0])
    for came in arrivals[1:]:
        came, keep_came = parted(came)
        total = total + weight * came
        weight = weight * keep_came
    after_early = keep_early * total + early
    stay = jnp.where(is_first, total, after_early).astype(bf16)
    got = swap(jnp.where(is_first, after_early, total).astype(bf16))
    return stay, got, gate, mixed


def local(
    hidden_in,
    doc_ids,
    norm_gain,
    in_zx,
    in_bc,
    in_dt,
    conv_x,
    conv_bc,
    bias_x,
    bias_bc,
    dt_bias,
    a_log,
    d_skip,
    gated_gain,
    out_w,
):
    route = Route(tuple(lax.axis_size(a) for a in AXES))
    section = lax.axis_index("pipe")
    tp = lax.axis_index("tp")
    micro_count = hidden_in.shape[0]
    channels = gated_gain.shape[1]
    local_heads = dt_bias.shape[1]
    width = channels // local_heads
    depth = in_zx.shape[1]
    rows = doc_ids.shape[1]
    own_rows = hidden_in.shape[1]
    state_width = in_bc.shape[2] // 2
    heads = 8 if local_heads % 8 == 0 else local_heads
    tiles = local_heads // heads
    sizes = (rows, heads, width, tiles, state_width)
    full_width = channels * route.tps

    def lanes(a):
        return jnp.pad(a, ((0, 0), (0, LANES - local_heads)))

    w_zx = in_zx[0].reshape(depth, 2 * channels)
    wdt = jnp.pad(in_dt[0].T, ((0, LANES - local_heads), (0, 0)))
    dtb = lanes(dt_bias)
    rate = lanes(-jnp.exp(a_log))
    skip = jnp.repeat(d_skip, width, axis=1)
    every = route.every()
    outputs = []
    for micro in range(micro_count):
        ids = doc_ids[micro].astype(f32)
        ids_row = jnp.broadcast_to(
            jnp.pad(ids[rows - 8 :], (0, depth - 8)).astype(bf16)[None, :], (HALO, depth)
        )
        current = hidden_in[micro]
        source = 0
        result = jnp.zeros_like(current)
        for pipe in range(route.pipes):
            if source == pipe:
                parts, halos = gather_rows(route, current, source, pipe, None, ids_row)
                before = sum(h[HALO, :8].astype(f32) for h in halos)
                before = jnp.where(lax.axis_index("seq") == 0, -1.0, before)
                idc = jnp.broadcast_to(
                    jnp.concatenate([before, ids])[:, None], (rows + 8, LANES)
                )
                idr = jnp.broadcast_to(ids[None, :], (8, rows))
            else:
                parts, halos = gather_rows(route, current, source, pipe)
            residual = parts[0]
            at = ((tp + jnp.arange(route.tps, dtype=jnp.int32)) % route.tps) * own_rows
            normed, x, bc, acol, arow, srow, ein, eall, states, sent = scan_call(
                at,
                parts,
                halos,
                norm_gain,
                in_bc[0],
                wdt,
                w_zx,
                conv_x[0],
                conv_bc[0],
                bias_x,
                bias_bc,
                dtb,
                rate,
                idc,
                sizes,
            )
            stay, got, gate, y = exchange_states(
                route,
                sent,
                state_width,
                pipe,
                lambda: gate_call(normed, w_zx, sizes),
                lambda a: inner_call(a, bc, acol, arow, srow, ein, states, skip, idc, idr, sizes),
                (x,),
            )
            swapped = lax.axis_index("seq") % 2
            total = None
            squares = None
            for distance in range(1, route.tps):
                at = jnp.stack([(tp + distance) % route.tps, swapped]).astype(jnp.int32)
                part, sq = out_call(
                    at, y, gate, bc, eall, stay, got, gated_gain, out_w[0], own_rows, sizes
                )
                pairs = [
                    ((pipe, s, t), (pipe, s, (t + distance) % route.tps)) for s, t in every
                ]
                part = route.move(part, pairs).astype(f32)
                sq = route.move(sq, pairs)
                total = part if total is None else total + part
                squares = sq if squares is None else squares + sq
            part, sq = out_call(
                jnp.stack([tp, swapped]).astype(jnp.int32),
                y, gate, bc, eall, stay, got, gated_gain, out_w[0], own_rows, sizes
            )
            total = part.astype(f32) if total is None else total + part.astype(f32)
            squares = sq if squares is None else squares + sq
            scale = lax.rsqrt(squares[:, 0:1] / full_width + epsilon)
            current = (residual.astype(f32) + scale * total).astype(bf16)
            source = pipe
            result = jnp.where(section == pipe, current, result)
        outputs.append(result)
    return jnp.stack(outputs)[None]


def solution(mesh):
    placed = (
        P(None, ("seq", "tp"), None),
        P(None, "seq"),
        P("pipe", None),
        P("pipe", None, None, "tp"),
        P("pipe", None, None),
        P("pipe", None, "tp"),
        P("pipe", None, "tp"),
        P("pipe", None, None),
        P("pipe", "tp"),
        P("pipe", None),
        P("pipe", "tp"),
        P("pipe", "tp"),
        P("pipe", "tp"),
        P("pipe", "tp"),
        P("pipe", "tp", None),
    )
    return jax.shard_map(
        local,
        mesh=mesh,
        in_specs=placed,
        out_specs=P("pipe", None, ("seq", "tp"), None),
        check_vma=False,
    )
```
